32 devices in a mesh: dp: 4 (over y, z), tp: 8 (over x, core).
Axes of the slice: x: 4, y: 2, z: 2, core: 2. Of those that a mesh axis runs over, the one named last changes fastest.
The devices are a block of a 4x4x8 slice.
Arguments:
- x_tokens: bfloat16 [12, 384, 3072], P('dp', 'tp'), parts along dimension 0
- start_pos: int32 [12], P('dp'), parts along dimension 0
- k_cache: bfloat16 [2, 12, 8, 3456, 128], P(None, 'dp', 'tp'), parts along dimension 1
- v_cache: bfloat16 [2, 12, 8, 3456, 128], P(None, 'dp', 'tp'), parts along dimension 1
- w_q: bfloat16 [2, 3072, 4096], P(None, None, 'tp')
- w_k: bfloat16 [2, 3072, 1024], P(None, None, 'tp')
- w_v: bfloat16 [2, 3072, 1024], P(None, None, 'tp')
- w_o: bfloat16 [2, 4096, 3072], P(None, 'tp')
- w_up: bfloat16 [2, 3072, 9216], P(None, None, 'tp')
- w_down: bfloat16 [2, 9216, 3072], P(None, 'tp')
- ln_gain: bfloat16 [2, 2, 3072], replicated
- ln_bias: bfloat16 [2, 2, 3072], replicated
Outputs:
- output 1: bfloat16 [12, 384, 3072], P('dp', 'tp'), parts along dimension 0
- output 2: bfloat16 [2, 12, 8, 3456, 128], P(None, 'dp', 'tp'), parts along dimension 1
- output 3: bfloat16 [2, 12, 8, 3456, 128], P(None, 'dp', 'tp'), parts along dimension 1
There are 4 independent parts. The reference program is written for one: setup_inputs(seed, part) draws one part's arguments, and reference() takes and returns one part's arrays. A program takes and returns all parts, laid end to end along the dimension named above; an argument that names none is the same for every part.
All inputs are finite; a program needn't handle non-finite values.
Results may differ from the reference program's by a relative error of at most 0.02.
Values are sent between devices in bfloat16 or wider.
A program may use at most 768 MiB of HBM per device.

```python
import jax
import jax.numpy as jnp
from jax import lax

LAYERS = 2
BATCH_SEQS = 3
NEW_TOKENS = 384
PREFIX_MAX = 3072
D_MODEL = 3072
N_HEADS = 32
KV_HEADS = 8
HEAD_DIM = 128
FF_DIM = 9216

CACHE_LEN = PREFIX_MAX + NEW_TOKENS
Q_WIDTH = N_HEADS * HEAD_DIM
KV_WIDTH = KV_HEADS * HEAD_DIM
GROUP_SIZE = N_HEADS // KV_HEADS
ROT_DIM = HEAD_DIM // 2
LN_EPS = 1e-5
ROPE_BASE = 10000.0
SOFTMAX_SCALE = HEAD_DIM ** -0.5
NEG_BIG = -1e30


def draw_weight(key_w, shape, fan_in, gain):
    return (jax.random.normal(key_w, shape, jnp.float32) * (gain * fan_in ** -0.5)).astype(jnp.bfloat16)


def draw_starts(key_s):
    key_low, key_pick = jax.random.split(key_s)
    low_bound = PREFIX_MAX // 4
    drawn = jax.random.randint(key_low, (BATCH_SEQS,), low_bound, PREFIX_MAX + 1, jnp.int32)
    chosen = jax.random.randint(key_pick, (), 0, BATCH_SEQS, jnp.int32)
    return jnp.where(jnp.arange(BATCH_SEQS, dtype=jnp.int32) == chosen, PREFIX_MAX, drawn).astype(jnp.int32)


def setup_inputs(seed: int = 0, part: int = 0) -> dict:
    part_key = jax.random.fold_in(jax.random.key(seed), part)
    part_keys = jax.random.split(part_key, 4)
    weight_keys = jax.random.split(jax.random.key(seed + 1), 8)
    cache_shape = (LAYERS, BATCH_SEQS, KV_HEADS, CACHE_LEN, HEAD_DIM)
    return {
        'x_tokens': jax.random.normal(part_keys[0], (BATCH_SEQS, NEW_TOKENS, D_MODEL), jnp.float32).astype(jnp.bfloat16),
        'start_pos': draw_starts(part_keys[1]),
        'k_cache': jax.random.normal(part_keys[2], cache_shape, jnp.float32).astype(jnp.bfloat16),
        'v_cache': jax.random.normal(part_keys[3], cache_shape, jnp.float32).astype(jnp.bfloat16),
        'w_q': draw_weight(weight_keys[0], (LAYERS, D_MODEL, Q_WIDTH), D_MODEL, 1.5),
        'w_k': draw_weight(weight_keys[1], (LAYERS, D_MODEL, KV_WIDTH), D_MODEL, 1.0),
        'w_v': draw_weight(weight_keys[2], (LAYERS, D_MODEL, KV_WIDTH), D_MODEL, 1.0),
        'w_o': draw_weight(weight_keys[3], (LAYERS, Q_WIDTH, D_MODEL), Q_WIDTH, 3.0),
        'w_up': draw_weight(weight_keys[4], (LAYERS, D_MODEL, FF_DIM), D_MODEL, 1.0),
        'w_down': draw_weight(weight_keys[5], (LAYERS, FF_DIM, D_MODEL), FF_DIM, 1.0),
        'ln_gain': (0.3 * jax.random.normal(weight_keys[6], (LAYERS, 2, D_MODEL), jnp.float32)).astype(jnp.bfloat16),
        'ln_bias': (0.3 * jax.random.normal(weight_keys[7], (LAYERS, 2, D_MODEL), jnp.float32)).astype(jnp.bfloat16),
    }


def layer_norm1p(values_in, gain, bias):
    x_float = values_in.astype(jnp.float32)
    row_mean = jnp.mean(x_float, axis=-1, keepdims=True)
    centered = x_float - row_mean
    variance = jnp.mean(centered * centered, axis=-1, keepdims=True)
    normed = centered * lax.rsqrt(variance + LN_EPS)
    return (normed * (1.0 + gain.astype(jnp.float32)) + bias.astype(jnp.float32)).astype(jnp.bfloat16)


def rotate_half(values_in, positions):
    half_rot = ROT_DIM // 2
    inv_freq = ROPE_BASE ** (-(jnp.arange(half_rot, dtype=jnp.float32) * (2.0 / ROT_DIM)))
    angles = positions.astype(jnp.float32)[..., None] * inv_freq
    cos_a = jnp.cos(angles)
    sin_a = jnp.sin(angles)
    first = values_in[..., :half_rot]
    second = values_in[..., half_rot:ROT_DIM]
    return jnp.concatenate([first * cos_a - second * sin_a, second * cos_a + first * sin_a, values_in[..., ROT_DIM:]], axis=-1)


def write_rows(cache_seq, new_rows, start_row):
    zero_idx = jnp.zeros_like(start_row)
    return lax.dynamic_update_slice(cache_seq, new_rows, (zero_idx, start_row, zero_idx))


def attend_one(item):
    q_seq, k_seq, v_seq, pos_seq = item
    key_ok = jnp.arange(CACHE_LEN, dtype=jnp.int32)[None, :] <= pos_seq[:, None]
    q_heads = jnp.transpose(q_seq, (1, 2, 0, 3))

    def one_head(head_item):
        q_head, k_head, v_head = head_item
        scores = jnp.einsum('gch,sh->gcs', q_head.astype(jnp.float32), k_head.astype(jnp.float32)) * SOFTMAX_SCALE
        scores = jnp.where(key_ok[None], scores, NEG_BIG)
        peak = jnp.max(scores, axis=-1, keepdims=True)
        weights = jnp.exp(scores - peak)
        row_sum = jnp.sum(weights, axis=-1, keepdims=True)
        context = jnp.einsum('gcs,sh->gch', weights.astype(jnp.bfloat16).astype(jnp.float32), v_head.astype(jnp.float32)) / row_sum
        return context.astype(jnp.bfloat16)

    ctx_heads = lax.map(one_head, (q_heads, k_seq, v_seq))
    return jnp.transpose(ctx_heads, (2, 0, 1, 3))


def reference(x_tokens, start_pos, k_cache, v_cache, w_q, w_k, w_v, w_o, w_up, w_down, ln_gain, ln_bias):
    positions = start_pos[:, None] + jnp.arange(NEW_TOKENS, dtype=jnp.int32)[None, :]
    rows_all = BATCH_SEQS * NEW_TOKENS

    def layer_step(hidden, layer_args):
        q_weight, k_weight, v_weight, o_weight, up_weight, down_weight, k_old, v_old, gain_pair, bias_pair = layer_args
        normed = layer_norm1p(hidden, gain_pair[0], bias_pair[0]).reshape(rows_all, D_MODEL)
        q_proj = jnp.dot(normed, q_weight, preferred_element_type=jnp.float32).reshape(BATCH_SEQS, NEW_TOKENS, N_HEADS, HEAD_DIM)
        k_proj = jnp.dot(normed, k_weight, preferred_element_type=jnp.float32).reshape(BATCH_SEQS, NEW_TOKENS, KV_HEADS, HEAD_DIM)
        v_proj = jnp.dot(normed, v_weight, preferred_element_type=jnp.float32).astype(jnp.bfloat16).reshape(BATCH_SEQS, NEW_TOKENS, KV_HEADS, HEAD_DIM)
        q_rot = rotate_half(q_proj, positions[:, :, None]).astype(jnp.bfloat16)
        k_rot = rotate_half(k_proj, positions[:, :, None]).astype(jnp.bfloat16)
        k_new = jax.vmap(write_rows)(k_old, jnp.transpose(k_rot, (0, 2, 1, 3)), start_pos)
        v_new = jax.vmap(write_rows)(v_old, jnp.transpose(v_proj, (0, 2, 1, 3)), start_pos)
        q_grouped = q_rot.reshape(BATCH_SEQS, NEW_TOKENS, KV_HEADS, GROUP_SIZE, HEAD_DIM)
        context = lax.map(attend_one, (q_grouped, k_new, v_new, positions)).reshape(rows_all, Q_WIDTH)
        attn_out = jnp.dot(context, o_weight, preferred_element_type=jnp.float32).astype(jnp.bfloat16).reshape(BATCH_SEQS, NEW_TOKENS, D_MODEL)
        after_attn = (hidden.astype(jnp.float32) + attn_out.astype(jnp.float32)).astype(jnp.bfloat16)
        normed_mlp = layer_norm1p(after_attn, gain_pair[1], bias_pair[1]).reshape(rows_all, D_MODEL)
        up_val = jnp.dot(normed_mlp, up_weight, preferred_element_type=jnp.float32)
        act_sq = jnp.square(jnp.maximum(up_val, 0.0)).astype(jnp.bfloat16)
        mlp_out = jnp.dot(act_sq, down_weight, preferred_element_type=jnp.float32).astype(jnp.bfloat16).reshape(BATCH_SEQS, NEW_TOKENS, D_MODEL)
        new_hidden = (after_attn.astype(jnp.float32) + mlp_out.astype(jnp.float32)).astype(jnp.bfloat16)
        return new_hidden, (k_new, v_new)

    hidden_out, caches_out = lax.scan(layer_step, x_tokens, (w_q, w_k, w_v, w_o, w_up, w_down, k_cache, v_cache, ln_gain, ln_bias))
    return (hidden_out, caches_out[0], caches_out[1])
```

```python
import functools
import math

import jax
import jax.numpy as jnp
from jax import lax
from jax.experimental import pallas as pl
from jax.experimental.pallas import tpu as pltpu
from jax.sharding import PartitionSpec as P

LN_EPS = 1e-5
ROPE_BASE = 10000.0
NEG_BIG = -1e30
CORES = 2
CHIPS = 4
GSLOTS = 3


def rope_tables(positions, head_dim):
    rot_dim = head_dim // 2
    half_rot = rot_dim // 2
    inv_freq = ROPE_BASE ** (-(jnp.arange(half_rot, dtype=jnp.float32) * (2.0 / rot_dim)))
    angles = positions.astype(jnp.float32)[..., None] * inv_freq
    cos_a = jnp.cos(angles)
    sin_a = jnp.sin(angles)
    ones = jnp.ones(cos_a.shape[:-1] + (head_dim - rot_dim,), jnp.float32)
    zeros_r = jnp.zeros_like(ones)
    zeros_h = jnp.zeros_like(sin_a)
    cos_t = jnp.concatenate([cos_a, cos_a, ones], axis=-1)
    sin_lo = jnp.concatenate([-sin_a, zeros_h, zeros_r], axis=-1)
    sin_hi = jnp.concatenate([zeros_h, sin_a, zeros_r], axis=-1)
    return cos_t, sin_lo, sin_hi


def layers_kernel(dims, start_ref, x_ref, gain_ref, bias_ref, cos_ref, slo_ref, shi_ref, kc_ref, vc_ref,
                  wq_ref, wk_ref, wv_ref, wo_ref, wu_ref, wd_ref,
                  xo_ref, kn_ref, vn_ref,
                  gath, part, pairin, pair, d2in, fin, wqkv, wov, wuv, wdv, kbuf, vbuf, qbuf, cbuf, abuf, sbuf, pbuf,
                  ag_s, ag_r, dd_s, dd_r, d2_s, d2_r, f_s, f_r, w_sem, kv_sem, kn_sem):
    n_layers, n_seq, tok, d_model, heads, head_dim, prefix, ff = dims
    new_len = tok * CORES * CHIPS
    half = d_model // 2
    steps = n_layers * 2 * n_seq
    tp_idx = lax.axis_index('tp')
    chip = tp_idx // CORES
    core = tp_idx % CORES
    sib = 1 - core
    rchip = (chip + 1) % CHIPS
    lchip = (chip + CHIPS - 1) % CHIPS
    ochip = (chip + 2) % CHIPS
    right = {'tp': rchip * CORES + core}
    left = {'tp': lchip * CORES + core}
    sibling = {'tp': chip * CORES + sib}
    lo = pl.ds(0, half)
    hi = pl.ds(half, half)

    def remote(src, dst, s_sem, r_sem, dev):
        return pltpu.make_async_remote_copy(src_ref=src, dst_ref=dst, send_sem=s_sem, recv_sem=r_sem,
                                            device_id=dev, device_id_type=pl.DeviceIdType.MESH)

    def ag_copy(m, k):
        g = m % GSLOTS
        where_from = [(chip, core, lo, right), (chip, core, hi, right), (chip, core, hi, left), (chip, core, lo, left),
                      (chip, core, None, sibling), (lchip, core, lo, right), (rchip, core, hi, left),
                      (lchip, core, None, sibling), (rchip, core, None, sibling), (ochip, core, lo, sibling),
                      (ochip, core, hi, sibling)]
        c, r, cols, dev = where_from[k]
        ref = gath.at[g, c, r] if cols is None else gath.at[g, c, r, :, cols]
        return remote(ref, ref, ag_s.at[g, k], ag_r.at[g, k], dev)

    def ag_start(m, ks):
        for k in ks:
            ag_copy(m, k).start()

    def ag_wait_recv(m, ks):
        for k in ks:
            ag_copy(m, k).wait_recv()

    def dd_copy():
        return remote(part.at[:, sib], pairin, dd_s, dd_r, sibling)

    def d2_copy(n, k):
        p = n % 2
        cols, dev = [(lo, right), (hi, left)][k]
        return remote(pair.at[p, ochip, :, cols], d2in.at[p, k], d2_s.at[p, k], d2_r.at[p, k], dev)

    def f_copy(n, k):
        p = n % 2
        f = n % 3
        c, cols, side, dev = [(rchip, hi, 0, right), (rchip, lo, 0, right), (lchip, lo, 1, left), (lchip, hi, 1, left)][k]
        return remote(pair.at[p, c, :, cols], fin.at[f, side, :, cols], f_s.at[f, k], f_r.at[f, k], dev)

    def attn_weights(l):
        qw = heads * head_dim
        return [pltpu.make_async_copy(wq_ref.at[l], wqkv.at[:, pl.ds(0, qw)], w_sem.at[0]),
                pltpu.make_async_copy(wk_ref.at[l], wqkv.at[:, pl.ds(qw, head_dim)], w_sem.at[1]),
                pltpu.make_async_copy(wv_ref.at[l], wqkv.at[:, pl.ds(qw + head_dim, head_dim)], w_sem.at[2]),
                pltpu.make_async_copy(wo_ref.at[l], wov, w_sem.at[3])]

    def mlp_weights(l):
        return [pltpu.make_async_copy(wu_ref.at[l], wuv, w_sem.at[4]),
                pltpu.make_async_copy(wd_ref.at[l], wdv, w_sem.at[5])]

    def kv_loads(a):
        l, b, p = a // n_seq, a % n_seq, a % 2
        rows = pl.ds(0, prefix)
        return [pltpu.make_async_copy(kc_ref.at[l, b, 0, rows], kbuf.at[p, rows], kv_sem.at[p, 0]),
                pltpu.make_async_copy(vc_ref.at[l, b, 0, rows], vbuf.at[p, rows], kv_sem.at[p, 1])]

    def start(copies):
        for c in copies:
            c.start()

    def wait(copies):
        for c in copies:
            c.wait()

    def norm_into(b, idx, m):
        xf = xo_ref[b].astype(jnp.float32)
        mean = jnp.sum(xf, axis=-1, keepdims=True) * (1.0 / d_model)
        cen = xf - mean
        var = jnp.sum(cen * cen, axis=-1, keepdims=True) * (1.0 / d_model)
        out = cen * lax.rsqrt(var + LN_EPS) * gain_ref[idx] + bias_ref[idx]
        gath[m % GSLOTS, chip, core] = out.astype(jnp.bfloat16)

    def pair_sum(n):
        dd_copy().wait()
        for k in range(11):
            ag_copy(n, k).wait_send()

        @pl.when(n >= 2)
        def _():
            for k in range(2):
                d2_copy(n - 2, k).wait_send()
            for k in range(4):
                f_copy(n - 2, k).wait_send()

        p = n % 2

        def add(c):
            pair[p, c] = (part[c, core].astype(jnp.float32) + pairin[c].astype(jnp.float32)).astype(jnp.bfloat16)

        add(ochip)
        d2_copy(n, 0).start()
        d2_copy(n, 1).start()
        add(rchip)
        f_copy(n, 0).start()
        add(lchip)
        f_copy(n, 2).start()
        add(chip)

    def add_through(n):
        p = n % 2
        d2_copy(n, 0).wait_recv()
        pair[p, rchip, :, lo] = (pair[p, rchip, :, lo].astype(jnp.float32) + d2in[p, 0].astype(jnp.float32)).astype(jnp.bfloat16)
        f_copy(n, 1).start()
        d2_copy(n, 1).wait_recv()
        pair[p, lchip, :, hi] = (pair[p, lchip, :, hi].astype(jnp.float32) + d2in[p, 1].astype(jnp.float32)).astype(jnp.bfloat16)
        f_copy(n, 3).start()

    def finalize(n):
        for k in range(4):
            f_copy(n, k).wait_recv()
        p = n % 2
        f = n % 3
        b = n % n_seq
        o = pair[p, chip].astype(jnp.float32) + fin[f, 0].astype(jnp.float32) + fin[f, 1].astype(jnp.float32)
        o = o.astype(jnp.bfloat16).astype(jnp.float32)
        xo_ref[b] = (xo_ref[b].astype(jnp.float32) + o).astype(jnp.bfloat16)

    def forward(m):
        ag_wait_recv(m, (0,))
        ag_start(m, (5,))
        ag_wait_recv(m, (2,))
        ag_start(m, (6,))
        ag_wait_recv(m, (1,))
        ag_start(m, (7,))
        ag_wait_recv(m, (3,))
        ag_start(m, (8,))

    def forward_far(m):
        ag_wait_recv(m, (5,))
        ag_start(m, (9,))
        ag_wait_recv(m, (6,))
        ag_start(m, (10,))

    def gathered(n):
        ag_wait_recv(n, (4, 7, 8, 9, 10))

    def event_add(n):
        @pl.when(n >= 1)
        def _():
            add_through(n - 1)

    def event_forward(n):
        @pl.when(n + 1 < steps)
        def _():
            forward(n + 1)

    def after_compute(n):
        dd_copy().start()
        pair_sum(n)

        @pl.when(n >= 1)
        def _():
            finalize(n - 1)

            @pl.when(n + 2 < steps)
            def _():
                norm_into((n + 2) % n_seq, (n + 2) // n_seq, n + 2)
                ag_start(n + 2, range(5))

        @pl.when(n + 1 < steps)
        def _():
            forward_far(n + 1)

    def rows_of(g):
        return gath[g].reshape(new_len, d_model)

    def put_part(cols, val):
        part[:, :, :, cols] = val.astype(jnp.bfloat16).reshape(CHIPS, CORES, tok, val.shape[-1])

    NT = (((1,), (1,)), ((), ()))
    tile = 256

    def attn_step(l, b, n):
        a = l * n_seq + b
        p = a % 2
        wait(kv_loads(a))

        @pl.when(a + 1 < n_layers * n_seq)
        def _():
            start(kv_loads(a + 1))

        gathered(n)
        g = n % GSLOTS
        cos_t, sin_lo, sin_hi = cos_ref[b], slo_ref[b], shi_ref[b]
        quarter = head_dim // 4

        def rotate(val):
            return (val * cos_t + pltpu.roll(val, head_dim - quarter, 1) * sin_lo + pltpu.roll(val, quarter, 1) * sin_hi).astype(jnp.bfloat16)

        kv = jnp.dot(rows_of(g), wqkv[:, pl.ds(heads * head_dim, 2 * head_dim)], preferred_element_type=jnp.float32)
        kbuf[p, pl.ds(prefix, new_len)] = rotate(kv[:, :head_dim])
        vbuf[p, pl.ds(prefix, new_len)] = kv[:, head_dim:].astype(jnp.bfloat16)
        outs = [pltpu.make_async_copy(kbuf.at[p, pl.ds(prefix, new_len)], kn_ref.at[l, b], kn_sem.at[0]),
                pltpu.make_async_copy(vbuf.at[p, pl.ds(prefix, new_len)], vn_ref.at[l, b], kn_sem.at[1])]
        start(outs)

        @pl.loop(0, heads // 2)
        def _(j):
            q2 = jnp.dot(rows_of(g), wqkv[:, pl.ds(pl.multiple_of(j * tile, tile), tile)], preferred_element_type=jnp.float32)
            qbuf[2 * j] = rotate(q2[:, :head_dim])
            qbuf[2 * j + 1] = rotate(q2[:, head_dim:])

        event_add(n)
        first_len = start_ref[b]
        chunk = math.gcd(prefix, 512)
        chunks = [(c, chunk) for c in range(0, prefix, chunk)] + [(prefix, new_len)]
        c_exp = head_dim ** -0.5 * math.log2(math.e)
        neg = NEG_BIG * head_dim ** 0.5

        @pl.loop(0, heads)
        def _(h):
            q = qbuf[h]
            peak = None
            for c0, cl in chunks:
                s = lax.dot_general(q, kbuf[p, pl.ds(c0, cl)], NT, preferred_element_type=jnp.float32)
                col = lax.broadcasted_iota(jnp.int32, (new_len, cl), 1)
                if c0 >= prefix:
                    s = jnp.where(col <= lax.broadcasted_iota(jnp.int32, (new_len, cl), 0), s, neg)
                else:
                    s = jnp.where(col < first_len - c0, s, neg)
                sbuf[:, pl.ds(c0, cl)] = s
                for k in range(0, cl, 128):
                    piece = s[:, k:k + 128]
                    peak = piece if peak is None else jnp.maximum(peak, piece)
            peak = jnp.max(peak, axis=-1, keepdims=True)
            total = None
            for c0, cl in chunks:
                e = jnp.exp2((sbuf[:, pl.ds(c0, cl)] - peak) * c_exp)
                pbuf[:, pl.ds(c0, cl)] = e.astype(jnp.bfloat16)
                for k in range(0, cl, 128):
                    piece = e[:, k:k + 128]
                    total = piece if total is None else total + piece
            total = jnp.sum(total, axis=-1, keepdims=True)
            ctx = jnp.dot(pbuf[...], vbuf[p], preferred_element_type=jnp.float32) / total
            cbuf[:, pl.ds(pl.multiple_of(h * head_dim, head_dim), head_dim)] = ctx.astype(jnp.bfloat16)

            @pl.when(h == 1)
            def _():
                event_forward(n)

        @pl.loop(0, d_model // tile)
        def _(j):
            cols = pl.ds(pl.multiple_of(j * tile, tile), tile)
            put_part(cols, jnp.dot(cbuf[...], wov[:, cols], preferred_element_type=jnp.float32))

        wait(outs)
        after_compute(n)

    def mlp_step(n):
        gathered(n)
        g = n % GSLOTS

        def up(cols):
            val = jnp.dot(rows_of(g), wuv[:, cols], preferred_element_type=jnp.float32)
            val = jnp.maximum(val, 0.0)
            abuf[:, cols] = (val * val).astype(jnp.bfloat16)

        @pl.loop(0, ff // tile)
        def _(j):
            up(pl.ds(pl.multiple_of(j * tile, tile), tile))

        if ff % tile:
            up(pl.ds(ff - ff % tile, ff % tile))
        event_add(n)
        n_tiles = d_model // tile

        @pl.loop(0, n_tiles)
        def _(j):
            cols = pl.ds(pl.multiple_of(j * tile, tile), tile)
            put_part(cols, jnp.dot(abuf[...], wdv[:, cols], preferred_element_type=jnp.float32))

            @pl.when(j == n_tiles // 2)
            def _():
                event_forward(n)

        after_compute(n)

    start(attn_weights(0))
    start(kv_loads(0))
    start(mlp_weights(0))
    xo_ref[...] = x_ref[...]

    barrier = pltpu.get_barrier_semaphore()
    for dev in (left, right, sibling):
        pl.semaphore_signal(barrier, inc=1, device_id=dev, device_id_type=pl.DeviceIdType.MESH)
    pl.semaphore_wait(barrier, 3)
    for b in range(n_seq):
        norm_into(b, 0, b)
        ag_start(b, range(5))
    forward(0)
    forward_far(0)

    @pl.loop(0, n_layers)
    def _(l):
        @pl.when(l >= 1)
        def _():
            start(mlp_weights(l))

        wait(attn_weights(l))

        @pl.loop(0, n_seq)
        def _(b):
            attn_step(l, b, l * 2 * n_seq + b)

        @pl.when(l + 1 < n_layers)
        def _():
            start(attn_weights(l + 1))

        wait(mlp_weights(l))

        @pl.loop(0, n_seq)
        def _(b):
            mlp_step(l * 2 * n_seq + n_seq + b)

    add_through(steps - 1)
    finalize(steps - 1)
    for n in (steps - 2, steps - 1):
        for k in range(2):
            d2_copy(n, k).wait_send()
        for k in range(4):
            f_copy(n, k).wait_send()


def run_layers(start_pos, x_loc, k_cache, v_cache, w_q, w_k, w_v, w_o, w_up, w_down, ln_gain, ln_bias, new_len):
    n_layers, n_seq, _, cache_len, head_dim = k_cache.shape
    tok, d_model = x_loc.shape[1:]
    heads = w_q.shape[2] // head_dim
    prefix = cache_len - new_len
    ff = w_up.shape[2]
    bf, f32 = jnp.bfloat16, jnp.float32
    positions = start_pos[:, None] + jnp.arange(new_len, dtype=jnp.int32)[None, :]
    cos_t, sin_lo, sin_hi = rope_tables(positions, head_dim)
    gain = (1.0 + ln_gain.astype(f32)).reshape(n_layers * 2, 1, d_model)
    bias = ln_bias.astype(f32).reshape(n_layers * 2, 1, d_model)
    vm = pl.BlockSpec(memory_space=pltpu.VMEM)
    hb = pl.BlockSpec(memory_space=pl.ANY)
    dims = (n_layers, n_seq, tok, d_model, heads, head_dim, prefix, ff)
    dma = pltpu.SemaphoreType.DMA
    return pl.pallas_call(
        functools.partial(layers_kernel, dims),
        out_shape=(jax.ShapeDtypeStruct(x_loc.shape, bf),
                   jax.ShapeDtypeStruct((n_layers, n_seq, new_len, head_dim), bf),
                   jax.ShapeDtypeStruct((n_layers, n_seq, new_len, head_dim), bf)),
        in_specs=[pl.BlockSpec(memory_space=pltpu.SMEM)] + [vm] * 6 + [hb] * 8,
        out_specs=(vm, hb, hb),
        scratch_shapes=[
            pltpu.VMEM((GSLOTS, CHIPS, CORES, tok, d_model), bf),
            pltpu.VMEM((CHIPS, CORES, tok, d_model), bf),
            pltpu.VMEM((CHIPS, tok, d_model), bf),
            pltpu.VMEM((2, CHIPS, tok, d_model), bf),
            pltpu.VMEM((2, 2, tok, d_model // 2), bf),
            pltpu.VMEM((3, 2, tok, d_model), bf),
            pltpu.VMEM((d_model, (heads + 2) * head_dim), bf),
            pltpu.VMEM((heads * head_dim, d_model), bf),
            pltpu.VMEM((d_model, ff), bf),
            pltpu.VMEM((ff, d_model), bf),
            pltpu.VMEM((2, cache_len, head_dim), bf),
            pltpu.VMEM((2, cache_len, head_dim), bf),
            pltpu.VMEM((heads, new_len, head_dim), bf),
            pltpu.VMEM((new_len, heads * head_dim), bf),
            pltpu.VMEM((new_len, ff), bf),
            pltpu.VMEM((new_len, cache_len), f32),
            pltpu.VMEM((new_len, cache_len), bf),
            dma((GSLOTS, 11)), dma((GSLOTS, 11)), dma, dma, dma((2, 2)), dma((2, 2)), dma((3, 4)), dma((3, 4)),
            dma((6,)), dma((2, 2)), dma((2,)),
        ],
        compiler_params=pltpu.CompilerParams(collective_id=0, has_side_effects=True, vmem_limit_bytes=67043328),
        name='layers',
    )(start_pos, x_loc, gain, bias, cos_t, sin_lo, sin_hi, k_cache, v_cache, w_q, w_k, w_v, w_o, w_up, w_down)


def merge_kernel(new_len, cache_len, n_seq, start_ref, kc_ref, vc_ref, kn_ref, vn_ref, ko_ref, vo_ref):
    first = start_ref[lax.rem(pl.program_id(0), n_seq)]
    span = new_len + 16
    base = pl.multiple_of(jnp.minimum(first // 16 * 16, cache_len - span), 16)
    shift = first - base
    row = lax.broadcasted_iota(jnp.int32, (span, kc_ref.shape[-1]), 0)
    inside = jnp.logical_and(row >= shift, row < shift + new_len)
    for old, new, out in ((kc_ref, kn_ref, ko_ref), (vc_ref, vn_ref, vo_ref)):
        out[...] = old[...]
        fresh = new[0].astype(jnp.float32)
        fresh = jnp.concatenate([fresh, jnp.zeros((16, fresh.shape[-1]), jnp.float32)], axis=0)
        fresh = pltpu.roll(fresh, shift, 0)
        kept = old[0, pl.ds(base, span), :].astype(jnp.float32)
        out[0, pl.ds(base, span), :] = jnp.where(inside, fresh, kept).astype(jnp.bfloat16)


def merge_caches(start_pos, k_cache, v_cache, k_new, v_new):
    n_layers, n_seq, kv, cache_len, head_dim = k_cache.shape
    new_len = k_new.shape[2]
    blocks = n_layers * n_seq
    flat = lambda c: c.reshape(blocks, cache_len, head_dim)
    whole = pl.BlockSpec((1, cache_len, head_dim), lambda i, s: (i, 0, 0))
    fresh = pl.BlockSpec((1, new_len, head_dim), lambda i, s: (i, 0, 0))
    shape = jax.ShapeDtypeStruct((blocks, cache_len, head_dim), jnp.bfloat16)
    k_out, v_out = pl.pallas_call(
        functools.partial(merge_kernel, new_len, cache_len, n_seq),
        out_shape=(shape, shape),
        grid_spec=pltpu.PrefetchScalarGridSpec(num_scalar_prefetch=1, grid=(blocks,), in_specs=[whole, whole, fresh, fresh], out_specs=[whole, whole]),
        name='merge',
    )(start_pos, flat(k_cache), flat(v_cache), k_new.reshape(blocks, new_len, head_dim), v_new.reshape(blocks, new_len, head_dim))
    return k_out.reshape(k_cache.shape), v_out.reshape(v_cache.shape)


def solution(mesh):
    tp_size = mesh.shape['tp']
    assert tp_size == CORES * CHIPS
    tok_spec = P('dp', 'tp', None)
    cache_spec = P(None, 'dp', 'tp', None, None)
    col_spec = P(None, None, 'tp')
    row_spec = P(None, 'tp', None)

    def device_fn(x_loc, start_pos, k_cache, v_cache, w_q, w_k, w_v, w_o, w_up, w_down, ln_gain, ln_bias):
        hidden, k_new, v_new = run_layers(start_pos, x_loc, k_cache, v_cache, w_q, w_k, w_v, w_o, w_up, w_down, ln_gain, ln_bias, x_loc.shape[1] * tp_size)
        k_out, v_out = merge_caches(start_pos, k_cache, v_cache, k_new, v_new)
        return hidden, k_out, v_out

    return jax.shard_map(device_fn, mesh=mesh, in_specs=(tok_spec, P('dp'), cache_spec, cache_spec, col_spec, col_spec, col_spec, row_spec, col_spec, row_spec, P(), P()), out_specs=(tok_spec, cache_spec, cache_spec), check_vma=False)
```

```python
import functools
import math

import jax
import jax.numpy as jnp
from jax import lax
from jax.experimental import pallas as pl
from jax.experimental.pallas import tpu as pltpu
from jax.sharding import PartitionSpec as P

LN_EPS = 1e-5
ROPE_BASE = 10000.0
NEG_BIG = -1e30
CORES = 2
CHIPS = 4
GSLOTS = 3


def rope_freqs(head_dim):
    rot_dim = head_dim // 2
    half_rot = rot_dim // 2
    inv_freq = ROPE_BASE ** (-(jnp.arange(half_rot, dtype=jnp.float32) * (2.0 / rot_dim)))
    return jnp.tile(inv_freq, head_dim // half_rot)[None]


def layers_kernel(dims, start_ref, x_ref, lng_ref, lnb_ref, freq_ref, kc_ref, vc_ref,
                  wq_ref, wk_ref, wv_ref, wo_ref, wu_ref, wd_ref,
                  xo_ref, kn_ref, vn_ref,
                  gath, part, pairin, pair, d2in, fin, wqkv, wov, wuv, wdv, kbuf, vbuf, qbuf, cbuf, abuf, sbuf_a, sbuf_b,
                  gain_ref, bias_ref, cos_ref, slo_ref, shi_ref,
                  ag_s, ag_r, dd_s, dd_r, d2_s, d2_r, f_s, f_r, w_sem, kv_sem, kn_sem):
    n_layers, n_seq, tok, d_model, heads, head_dim, prefix, ff = dims
    new_len = tok * CORES * CHIPS
    half = d_model // 2
    steps = n_layers * 2 * n_seq
    tp_idx = lax.axis_index('tp')
    chip = tp_idx // CORES
    core = tp_idx % CORES
    sib = 1 - core
    rchip = (chip + 1) % CHIPS
    lchip = (chip + CHIPS - 1) % CHIPS
    ochip = (chip + 2) % CHIPS
    right = {'tp': rchip * CORES + core}
    left = {'tp': lchip * CORES + core}
    sibling = {'tp': chip * CORES + sib}
    lo = pl.ds(0, half)
    hi = pl.ds(half, half)

    def remote(src, dst, s_sem, r_sem, dev):
        return pltpu.make_async_remote_copy(src_ref=src, dst_ref=dst, send_sem=s_sem, recv_sem=r_sem,
                                            device_id=dev, device_id_type=pl.DeviceIdType.MESH)

    def ag_copy(m, k):
        g = m % GSLOTS
        where_from = [(chip, core, lo, right), (chip, core, hi, right), (chip, core, hi, left), (chip, core, lo, left),
                      (chip, core, None, sibling), (lchip, core, lo, right), (rchip, core, hi, left),
                      (lchip, core, None, sibling), (rchip, core, None, sibling), (ochip, core, lo, sibling),
                      (ochip, core, hi, sibling)]
        c, r, cols, dev = where_from[k]
        ref = gath.at[g, c, r] if cols is None else gath.at[g, c, r, :, cols]
        return remote(ref, ref, ag_s.at[g, k], ag_r.at[g, k], dev)

    def ag_start(m, ks):
        for k in ks:
            ag_copy(m, k).start()

    def ag_wait_recv(m, ks):
        for k in ks:
            ag_copy(m, k).wait_recv()

    def dd_copy(k):
        cols = (lo, hi)[k]
        return remote(part.at[:, sib, :, cols], pairin.at[:, :, cols], dd_s.at[k], dd_r.at[k], sibling)

    def d2_copy(n, k):
        p = n % 2
        cols, dev = [(lo, right), (hi, left)][k]
        return remote(pair.at[p, ochip, :, cols], d2in.at[p, k], d2_s.at[p, k], d2_r.at[p, k], dev)

    def f_copy(n, k):
        p = n % 2
        f = n % 3
        c, cols, side, dev = [(rchip, hi, 0, right), (rchip, lo, 0, right), (lchip, lo, 1, left), (lchip, hi, 1, left)][k]
        return remote(pair.at[p, c, :, cols], fin.at[f, side, :, cols], f_s.at[f, k], f_r.at[f, k], dev)

    def attn_weights(l):
        qw = heads * head_dim
        return [pltpu.make_async_copy(wq_ref.at[l], wqkv.at[:, pl.ds(0, qw)], w_sem.at[0]),
                pltpu.make_async_copy(wk_ref.at[l], wqkv.at[:, pl.ds(qw, head_dim)], w_sem.at[1]),
                pltpu.make_async_copy(wv_ref.at[l], wqkv.at[:, pl.ds(qw + head_dim, head_dim)], w_sem.at[2]),
                pltpu.make_async_copy(wo_ref.at[l], wov, w_sem.at[3])]

    def mlp_weights(l):
        return [pltpu.make_async_copy(wu_ref.at[l], wuv, w_sem.at[4]),
                pltpu.make_async_copy(wd_ref.at[l], wdv, w_sem.at[5])]

    def kv_loads(a):
        l, b, p = a // n_seq, a % n_seq, a % 2
        rows = pl.ds(0, prefix)
        return [pltpu.make_async_copy(kc_ref.at[l, b, 0, rows], kbuf.at[p, rows], kv_sem.at[p, 0]),
                pltpu.make_async_copy(vc_ref.at[l, b, 0, rows], vbuf.at[p, rows], kv_sem.at[p, 1])]

    def start(copies):
        for c in copies:
            c.start()

    def wait(copies):
        for c in copies:
            c.wait()

    def norm_into(b, idx, m):
        xf = xo_ref[b].astype(jnp.float32)
        mean = jnp.sum(xf, axis=-1, keepdims=True) * (1.0 / d_model)
        cen = xf - mean
        var = jnp.sum(cen * cen, axis=-1, keepdims=True) * (1.0 / d_model)
        out = cen * lax.rsqrt(var + LN_EPS) * gain_ref[idx] + bias_ref[idx]
        gath[m % GSLOTS, chip, core] = out.astype(jnp.bfloat16)

    def pair_sum(n):
        for k in range(11):
            ag_copy(n, k).wait_send()

        @pl.when(n >= 2)
        def _():
            for k in range(2):
                d2_copy(n - 2, k).wait_send()
            for k in range(4):
                f_copy(n - 2, k).wait_send()

        p = n % 2

        def add(c, cols):
            pair[p, c, :, cols] = (part[c, core, :, cols].astype(jnp.float32) + pairin[c, :, cols].astype(jnp.float32)).astype(jnp.bfloat16)

        for k, (cols, near, ready, far) in enumerate(((lo, lchip, 2, rchip), (hi, rchip, 0, lchip))):
            dd_copy(k).wait()
            add(ochip, cols)
            d2_copy(n, k).start()
            add(near, cols)
            f_copy(n, ready).start()
            add(far, cols)
            add(chip, cols)

    def add_through(n):
        p = n % 2
        d2_copy(n, 0).wait_recv()
        pair[p, rchip, :, lo] = (pair[p, rchip, :, lo].astype(jnp.float32) + d2in[p, 0].astype(jnp.float32)).astype(jnp.bfloat16)
        f_copy(n, 1).start()
        d2_copy(n, 1).wait_recv()
        pair[p, lchip, :, hi] = (pair[p, lchip, :, hi].astype(jnp.float32) + d2in[p, 1].astype(jnp.float32)).astype(jnp.bfloat16)
        f_copy(n, 3).start()

    def finalize(n):
        for k in range(4):
            f_copy(n, k).wait_recv()
        p = n % 2
        f = n % 3
        b = n % n_seq
        o = pair[p, chip].astype(jnp.float32) + fin[f, 0].astype(jnp.float32) + fin[f, 1].astype(jnp.float32)
        o = o.astype(jnp.bfloat16).astype(jnp.float32)
        xo_ref[b] = (xo_ref[b].astype(jnp.float32) + o).astype(jnp.bfloat16)

    def forward(m):
        ag_wait_recv(m, (0,))
        ag_start(m, (5,))
        ag_wait_recv(m, (2,))
        ag_start(m, (6,))
        ag_wait_recv(m, (1,))
        ag_start(m, (7,))
        ag_wait_recv(m, (3,))
        ag_start(m, (8,))

    def forward_far(m):
        ag_wait_recv(m, (5,))
        ag_start(m, (9,))
        ag_wait_recv(m, (6,))
        ag_start(m, (10,))

    def gathered(n):
        ag_wait_recv(n, (4, 7, 8, 9, 10))

    def event_add(n):
        @pl.when(n >= 1)
        def _():
            add_through(n - 1)

    def event_forward(n):
        @pl.when(n + 1 < steps)
        def _():
            forward(n + 1)

    def after_compute(n):
        pair_sum(n)

        @pl.when(n >= 1)
        def _():
            finalize(n - 1)

            @pl.when(n + 2 < steps)
            def _():
                norm_into((n + 2) % n_seq, (n + 2) // n_seq, n + 2)
                ag_start(n + 2, range(5))

        @pl.when(n + 1 < steps)
        def _():
            forward_far(n + 1)

    def rows_of(g):
        return gath[g].reshape(new_len, d_model)

    def put_part(cols, val):
        part[:, :, :, cols] = val.astype(jnp.bfloat16).reshape(CHIPS, CORES, tok, val.shape[-1])

    NT = (((1,), (1,)), ((), ()))
    tile = 256

    def product_into_part(lhs, weights):
        for k in range(2):
            @pl.loop(0, half // tile)
            def _(j):
                cols = pl.ds(pl.multiple_of(k * half + j * tile, tile), tile)
                put_part(cols, jnp.dot(lhs[...], weights[:, cols], preferred_element_type=jnp.float32))

            dd_copy(k).start()

    def attn_step(l, b, n):
        a = l * n_seq + b
        p = a % 2
        wait(kv_loads(a))

        @pl.when(a + 1 < n_layers * n_seq)
        def _():
            start(kv_loads(a + 1))

        gathered(n)
        g = n % GSLOTS
        cos_t, sin_lo, sin_hi = cos_ref[b], slo_ref[b], shi_ref[b]
        quarter = head_dim // 4

        def rotate(val):
            return (val * cos_t + pltpu.roll(val, head_dim - quarter, 1) * sin_lo + pltpu.roll(val, quarter, 1) * sin_hi).astype(jnp.bfloat16)

        kv = jnp.dot(rows_of(g), wqkv[:, pl.ds(heads * head_dim, 2 * head_dim)], preferred_element_type=jnp.float32)
        kbuf[p, pl.ds(prefix, new_len)] = rotate(kv[:, :head_dim])
        vbuf[p, pl.ds(prefix, new_len)] = kv[:, head_dim:].astype(jnp.bfloat16)
        outs = [pltpu.make_async_copy(kbuf.at[p, pl.ds(prefix, new_len)], kn_ref.at[l, b], kn_sem.at[0]),
                pltpu.make_async_copy(vbuf.at[p, pl.ds(prefix, new_len)], vn_ref.at[l, b], kn_sem.at[1])]
        start(outs)

        @pl.loop(0, heads // 2)
        def _(j):
            q2 = jnp.dot(rows_of(g), wqkv[:, pl.ds(pl.multiple_of(j * tile, tile), tile)], preferred_element_type=jnp.float32)
            qbuf[2 * j] = rotate(q2[:, :head_dim])
            qbuf[2 * j + 1] = rotate(q2[:, head_dim:])

        event_add(n)
        first_len = start_ref[b]
        chunk = prefix // 4
        chunks = [(c, chunk) for c in range(0, prefix, chunk)] + [(prefix, new_len)]
        c_exp = head_dim ** -0.5 * math.log2(math.e)
        neg = NEG_BIG * head_dim ** 0.5
        bufs = (sbuf_a, sbuf_b)

        def fold(old, val, op):
            for k in range(0, val.shape[-1], 128):
                piece = val[:, k:k + 128]
                old = piece if old is None else op(old, piece)
            return old

        def score_chunk(h, q, peak, c0, cl):
            s = lax.dot_general(q, kbuf[p, pl.ds(c0, cl)], NT, preferred_element_type=jnp.float32)
            if c0:
                col = lax.broadcasted_iota(jnp.int32, (new_len, cl), 1)
                last = lax.broadcasted_iota(jnp.int32, (new_len, cl), 0) if c0 >= prefix else first_len - c0 - 1
                s = jnp.where(col <= last, s, neg)
            bufs[h % 2][:, pl.ds(c0, cl)] = s
            return fold(peak, s, jnp.maximum)

        def weigh_chunk(h, peak, total, acc, c0, cl):
            e = jnp.exp2((bufs[h % 2][:, pl.ds(c0, cl)] - peak) * c_exp)
            part_ctx = jnp.dot(e.astype(jnp.bfloat16), vbuf[p, pl.ds(c0, cl)], preferred_element_type=jnp.float32)
            return fold(total, e, jnp.add), part_ctx if acc is None else acc + part_ctx

        peaks = None
        for h in range(heads + 1):
            if h == heads:
                event_forward(n)
            q = qbuf[h] if h < heads else None
            next_peak = total = acc = None
            for c0, cl in chunks:
                if h < heads:
                    next_peak = score_chunk(h, q, next_peak, c0, cl)
                if h:
                    total, acc = weigh_chunk(h - 1, peaks, total, acc, c0, cl)
            if h:
                ctx = acc / jnp.sum(total, axis=-1, keepdims=True)
                cbuf[:, pl.ds((h - 1) * head_dim, head_dim)] = ctx.astype(jnp.bfloat16)
            if h < heads:
                peaks = jnp.max(next_peak, axis=-1, keepdims=True)

        product_into_part(cbuf, wov)
        wait(outs)
        after_compute(n)

    def mlp_step(n):
        gathered(n)
        g = n % GSLOTS

        def up(cols):
            val = jnp.dot(rows_of(g), wuv[:, cols], preferred_element_type=jnp.float32)
            val = jnp.maximum(val, 0.0)
            abuf[:, cols] = (val * val).astype(jnp.bfloat16)

        @pl.loop(0, ff // tile)
        def _(j):
            up(pl.ds(pl.multiple_of(j * tile, tile), tile))

        if ff % tile:
            up(pl.ds(ff - ff % tile, ff % tile))
        event_add(n)
        product_into_part(abuf, wdv)
        event_forward(n)
        after_compute(n)

    start(attn_weights(0))
    start(kv_loads(0))
    xo_ref[...] = x_ref[...]
    for l in range(n_layers):
        for k in range(2):
            gain_ref[2 * l + k] = 1.0 + lng_ref[l, k:k + 1].astype(jnp.float32)
            bias_ref[2 * l + k] = lnb_ref[l, k:k + 1].astype(jnp.float32)

    barrier = pltpu.get_barrier_semaphore()
    for dev in (left, right, sibling):
        pl.semaphore_signal(barrier, inc=1, device_id=dev, device_id_type=pl.DeviceIdType.MESH)
    pl.semaphore_wait(barrier, 3)
    for b in range(n_seq):
        norm_into(b, 0, b)
        ag_start(b, range(5))
    lane = lax.broadcasted_iota(jnp.int32, (new_len, head_dim), 1)
    row = lax.broadcasted_iota(jnp.int32, (new_len, head_dim), 0)
    rot = head_dim // 2

    @pl.loop(0, n_seq)
    def _(b):
        angle = (start_ref[b] + row).astype(jnp.float32) * freq_ref[...]
        sin_a = jnp.sin(angle)
        cos_ref[b] = jnp.where(lane < rot, jnp.cos(angle), 1.0)
        slo_ref[b] = jnp.where(lane < rot // 2, -sin_a, 0.0)
        shi_ref[b] = jnp.where(jnp.logical_and(lane >= rot // 2, lane < rot), sin_a, 0.0)

    forward(0)
    forward_far(0)

    @pl.loop(0, n_layers)
    def _(l):
        wait(attn_weights(l))
        start(mlp_weights(l))

        @pl.loop(0, n_seq)
        def _(b):
            attn_step(l, b, l * 2 * n_seq + b)

        @pl.when(l + 1 < n_layers)
        def _():
            start(attn_weights(l + 1))

        wait(mlp_weights(l))

        @pl.loop(0, n_seq)
        def _(b):
            mlp_step(l * 2 * n_seq + n_seq + b)

    add_through(steps - 1)
    finalize(steps - 1)
    for n in (steps - 2, steps - 1):
        for k in range(2):
            d2_copy(n, k).wait_send()
        for k in range(4):
            f_copy(n, k).wait_send()


def run_layers(start_pos, x_loc, k_cache, v_cache, w_q, w_k, w_v, w_o, w_up, w_down, ln_gain, ln_bias, new_len):
    n_layers, n_seq, _, cache_len, head_dim = k_cache.shape
    tok, d_model = x_loc.shape[1:]
    heads = w_q.shape[2] // head_dim
    prefix = cache_len - new_len
    ff = w_up.shape[2]
    bf, f32 = jnp.bfloat16, jnp.float32
    vm = pl.BlockSpec(memory_space=pltpu.VMEM)
    hb = pl.BlockSpec(memory_space=pl.ANY)
    dims = (n_layers, n_seq, tok, d_model, heads, head_dim, prefix, ff)
    dma = pltpu.SemaphoreType.DMA
    return pl.pallas_call(
        functools.partial(layers_kernel, dims),
        out_shape=(jax.ShapeDtypeStruct(x_loc.shape, bf),
                   jax.ShapeDtypeStruct((n_layers, n_seq, new_len, head_dim), bf),
                   jax.ShapeDtypeStruct((n_layers, n_seq, new_len, head_dim), bf)),
        in_specs=[pl.BlockSpec(memory_space=pltpu.SMEM)] + [vm] * 4 + [hb] * 8,
        out_specs=(vm, hb, hb),
        scratch_shapes=[
            pltpu.VMEM((GSLOTS, CHIPS, CORES, tok, d_model), bf),
            pltpu.VMEM((CHIPS, CORES, tok, d_model), bf),
            pltpu.VMEM((CHIPS, tok, d_model), bf),
            pltpu.VMEM((2, CHIPS, tok, d_model), bf),
            pltpu.VMEM((2, 2, tok, d_model // 2), bf),
            pltpu.VMEM((3, 2, tok, d_model), bf),
            pltpu.VMEM((d_model, (heads + 2) * head_dim), bf),
            pltpu.VMEM((heads * head_dim, d_model), bf),
            pltpu.VMEM((d_model, ff), bf),
            pltpu.VMEM((ff, d_model), bf),
            pltpu.VMEM((2, cache_len, head_dim), bf),
            pltpu.VMEM((2, cache_len, head_dim), bf),
            pltpu.VMEM((heads, new_len, head_dim), bf),
            pltpu.VMEM((new_len, heads * head_dim), bf),
            pltpu.VMEM((new_len, ff), bf),
            pltpu.VMEM((new_len, cache_len), f32),
            pltpu.VMEM((new_len, cache_len), f32),
            pltpu.VMEM((n_layers * 2, 1, d_model), f32),
            pltpu.VMEM((n_layers * 2, 1, d_model), f32),
            pltpu.VMEM((n_seq, new_len, head_dim), f32),
            pltpu.VMEM((n_seq, new_len, head_dim), f32),
            pltpu.VMEM((n_seq, new_len, head_dim), f32),
            dma((GSLOTS, 11)), dma((GSLOTS, 11)), dma((2,)), dma((2,)), dma((2, 2)), dma((2, 2)), dma((3, 4)), dma((3, 4)),
            dma((6,)), dma((2, 2)), dma((2,)),
        ],
        compiler_params=pltpu.CompilerParams(collective_id=0, has_side_effects=True, vmem_limit_bytes=67043328),
        name='layers',
    )(start_pos, x_loc, ln_gain, ln_bias, rope_freqs(head_dim), k_cache, v_cache, w_q, w_k, w_v, w_o, w_up, w_down)


def merge_kernel(dims, start_ref, x_ref, kc_ref, vc_ref, kn_ref, vn_ref, xo_ref, ko_ref, vo_ref,
                 xbuf, kbuf, vbuf, knew, vnew, x_sem, in_sem, new_sem, out_sem):
    blocks, n_seq, new_len, cache_len, head_dim = dims
    span = new_len + 16
    row = lax.broadcasted_iota(jnp.int32, (span, head_dim), 0)
    caches = ((kc_ref, kbuf, kn_ref, knew, ko_ref), (vc_ref, vbuf, vn_ref, vnew, vo_ref))

    def reads(i, c):
        old, buf, new, nbuf, _ = caches[c]
        return (pltpu.make_async_copy(old.at[i], buf.at[i], in_sem.at[i, c]),
                pltpu.make_async_copy(new.at[i], nbuf.at[i], new_sem.at[i, c]))

    def write(i, c):
        return pltpu.make_async_copy(caches[c][1].at[i], caches[c][4].at[i], out_sem.at[i, c])

    for i in range(blocks):
        for c in range(2):
            for copy in reads(i, c):
                copy.start()
    x_in = pltpu.make_async_copy(x_ref, xbuf, x_sem.at[0])
    x_out = pltpu.make_async_copy(xbuf, xo_ref, x_sem.at[1])
    x_in.start()

    @pl.loop(0, blocks)
    def _(i):
        first = start_ref[lax.rem(i, n_seq)]
        base = pl.multiple_of(jnp.minimum(first // 16 * 16, cache_len - span), 16)
        shift = first - base
        inside = jnp.logical_and(row >= shift, row < shift + new_len)
        for c in range(2):
            for copy in reads(i, c):
                copy.wait()
            _, buf, _, nbuf, _ = caches[c]
            fresh = jnp.concatenate([nbuf[i].astype(jnp.float32), jnp.zeros((16, head_dim), jnp.float32)], axis=0)
            fresh = pltpu.roll(fresh, shift, 0)
            kept = buf[i, pl.ds(base, span), :].astype(jnp.float32)
            buf[i, pl.ds(base, span), :] = jnp.where(inside, fresh, kept).astype(jnp.bfloat16)
            write(i, c).start()

    x_in.wait()
    x_out.start()

    @pl.loop(0, blocks)
    def _(i):
        for c in range(2):
            write(i, c).wait()

    x_out.wait()


def merge_caches(start_pos, hidden, k_cache, v_cache, k_new, v_new):
    n_layers, n_seq, kv, cache_len, head_dim = k_cache.shape
    new_len = k_new.shape[2]
    blocks = n_layers * n_seq
    bf = jnp.bfloat16
    flat = lambda c: c.reshape(blocks, cache_len, head_dim)
    flat_new = lambda c: c.reshape(blocks, new_len, head_dim)
    hb = pl.BlockSpec(memory_space=pl.ANY)
    shape = jax.ShapeDtypeStruct((blocks, cache_len, head_dim), bf)
    dma = pltpu.SemaphoreType.DMA
    x_out, k_out, v_out = pl.pallas_call(
        functools.partial(merge_kernel, (blocks, n_seq, new_len, cache_len, head_dim)),
        out_shape=(jax.ShapeDtypeStruct(hidden.shape, bf), shape, shape),
        in_specs=[pl.BlockSpec(memory_space=pltpu.SMEM)] + [hb] * 5,
        out_specs=(hb, hb, hb),
        scratch_shapes=[pltpu.VMEM(hidden.shape, bf), pltpu.VMEM((blocks, cache_len, head_dim), bf), pltpu.VMEM((blocks, cache_len, head_dim), bf),
                        pltpu.VMEM((blocks, new_len, head_dim), bf), pltpu.VMEM((blocks, new_len, head_dim), bf),
                        dma((2,)), dma((blocks, 2)), dma((blocks, 2)), dma((blocks, 2))],
        name='merge',
    )(start_pos, hidden, flat(k_cache), flat(v_cache), flat_new(k_new), flat_new(v_new))
    return x_out, k_out.reshape(k_cache.shape), v_out.reshape(v_cache.shape)


def solution(mesh):
    tp_size = mesh.shape['tp']
    assert tp_size == CORES * CHIPS
    tok_spec = P('dp', 'tp', None)
    cache_spec = P(None, 'dp', 'tp', None, None)
    col_spec = P(None, None, 'tp')
    row_spec = P(None, 'tp', None)

    def device_fn(x_loc, start_pos, k_cache, v_cache, w_q, w_k, w_v, w_o, w_up, w_down, ln_gain, ln_bias):
        hidden, k_new, v_new = run_layers(start_pos, x_loc, k_cache, v_cache, w_q, w_k, w_v, w_o, w_up, w_down, ln_gain, ln_bias, x_loc.shape[1] * tp_size)
        return merge_caches(start_pos, hidden, k_cache, v_cache, k_new, v_new)

    return jax.shard_map(device_fn, mesh=mesh, in_specs=(tok_spec, P('dp'), cache_spec, cache_spec, col_spec, col_spec, col_spec, row_spec, col_spec, row_spec, P(), P()), out_specs=(tok_spec, cache_spec, cache_spec), check_vma=False)
```

```python
import functools
import math

import jax
import jax.numpy as jnp
import numpy as np
from jax import lax
from jax.experimental import pallas as pl
from jax.experimental.pallas import tpu as pltpu
from jax.sharding import PartitionSpec as P

LN_EPS = 1e-5
ROPE_BASE = 10000.0
NEG_BIG = -1e30
CORES = 2
CHIPS = 4
GSLOTS = 3


def rope_freqs(head_dim):
    rot_dim = head_dim // 2
    half_rot = rot_dim // 2
    inv_freq = ROPE_BASE ** (-(np.arange(half_rot) * (2.0 / rot_dim)))
    return jnp.asarray(np.tile(inv_freq, head_dim // half_rot)[None].astype(np.float32))


def layers_kernel(dims, start_ref, x_ref, lng_ref, lnb_ref, freq_ref, kc_ref, vc_ref,
                  wq_ref, wk_ref, wv_ref, wo_ref, wu_ref, wd_ref,
                  xo_ref, kn_ref, vn_ref,
                  gath, part, pairin, pair, d2in, fin, wqkv, wov, wuv, wdv, kbuf, vbuf, abuf, sbuf_a, sbuf_b,
                  gain_ref, bias_ref, cos_ref, slo_ref, shi_ref,
                  ag_s, ag_r, dd_s, dd_r, d2_s, d2_r, f_s, f_r, w_sem, kv_sem, kn_sem):
    n_layers, n_seq, tok, d_model, heads, head_dim, prefix, ff = dims
    new_len = tok * CORES * CHIPS
    half = d_model // 2
    steps = n_layers * 2 * n_seq
    tp_idx = lax.axis_index('tp')
    chip = tp_idx // CORES
    core = tp_idx % CORES
    sib = 1 - core
    rchip = (chip + 1) % CHIPS
    lchip = (chip + CHIPS - 1) % CHIPS
    ochip = (chip + 2) % CHIPS
    right = {'tp': rchip * CORES + core}
    left = {'tp': lchip * CORES + core}
    sibling = {'tp': chip * CORES + sib}
    lo = pl.ds(0, half)
    hi = pl.ds(half, half)

    def remote(src, dst, s_sem, r_sem, dev):
        return pltpu.make_async_remote_copy(src_ref=src, dst_ref=dst, send_sem=s_sem, recv_sem=r_sem,
                                            device_id=dev, device_id_type=pl.DeviceIdType.MESH)

    def ag_copy(m, k):
        g = m % GSLOTS
        where_from = [(chip, core, lo, right), (chip, core, hi, right), (chip, core, hi, left), (chip, core, lo, left),
                      (chip, core, None, sibling), (lchip, core, lo, right), (rchip, core, hi, left),
                      (lchip, core, None, sibling), (rchip, core, None, sibling), (ochip, core, lo, sibling),
                      (ochip, core, hi, sibling)]
        c, r, cols, dev = where_from[k]
        ref = gath.at[g, c, r] if cols is None else gath.at[g, c, r, :, cols]
        return remote(ref, ref, ag_s.at[g, k], ag_r.at[g, k], dev)

    def ag_start(m, ks):
        for k in ks:
            ag_copy(m, k).start()

    def ag_wait_recv(m, ks):
        for k in ks:
            ag_copy(m, k).wait_recv()

    def dd_copy(n, k):
        p = n % 2
        cols = (lo, hi)[k]
        return remote(part.at[:, sib, :, cols], pairin.at[p, :, :, cols], dd_s.at[p, k], dd_r.at[p, k], sibling)

    def d2_copy(n, k):
        p = n % 2
        cols, dev = [(lo, right), (hi, left)][k]
        return remote(pair.at[p, ochip, :, cols], d2in.at[p, k], d2_s.at[p, k], d2_r.at[p, k], dev)

    def f_copy(n, k):
        p = n % 2
        f = n % 3
        c, cols, side, dev = [(rchip, hi, 0, right), (rchip, lo, 0, right), (lchip, lo, 1, left), (lchip, hi, 1, left)][k]
        return remote(pair.at[p, c, :, cols], fin.at[f, side, :, cols], f_s.at[f, k], f_r.at[f, k], dev)

    def attn_weights(l):
        qw = heads * head_dim
        return [pltpu.make_async_copy(wq_ref.at[l], wqkv.at[:, pl.ds(0, qw)], w_sem.at[0]),
                pltpu.make_async_copy(wk_ref.at[l], wqkv.at[:, pl.ds(qw, head_dim)], w_sem.at[1]),
                pltpu.make_async_copy(wv_ref.at[l], wqkv.at[:, pl.ds(qw + head_dim, head_dim)], w_sem.at[2]),
                pltpu.make_async_copy(wo_ref.at[l], wov, w_sem.at[3])]

    def mlp_weights(l):
        return [pltpu.make_async_copy(wu_ref.at[l], wuv, w_sem.at[4]),
                pltpu.make_async_copy(wd_ref.at[l], wdv, w_sem.at[5])]

    def kv_loads(a):
        l, b, p = a // n_seq, a % n_seq, a % 2
        rows = pl.ds(0, prefix)
        return [pltpu.make_async_copy(kc_ref.at[l, b, 0, rows], kbuf.at[p, rows], kv_sem.at[p, 0]),
                pltpu.make_async_copy(vc_ref.at[l, b, 0, rows], vbuf.at[p, rows], kv_sem.at[p, 1])]

    def start(copies):
        for c in copies:
            c.start()

    def wait(copies):
        for c in copies:
            c.wait()

    def norm_into(b, idx, m):
        xf = xo_ref[b].astype(jnp.float32)
        mean = jnp.sum(xf, axis=-1, keepdims=True) * (1.0 / d_model)
        cen = xf - mean
        var = jnp.sum(cen * cen, axis=-1, keepdims=True) * (1.0 / d_model)
        out = cen * lax.rsqrt(var + LN_EPS) * gain_ref[idx] + bias_ref[idx]
        gath[m % GSLOTS, chip, core] = out.astype(jnp.bfloat16)

    def pair_sum(n, k):
        if k == 0:
            for i in range(11):
                ag_copy(n, i).wait_send()

            @pl.when(n >= 2)
            def _():
                for i in range(2):
                    d2_copy(n - 2, i).wait_send()
                for i in range(4):
                    f_copy(n - 2, i).wait_send()

        p = n % 2
        cols, near, far = ((lo, lchip, rchip), (hi, rchip, lchip))[k]

        def add(c):
            pair[p, c, :, cols] = (part[c, core, :, cols].astype(jnp.float32) + pairin[p, c, :, cols].astype(jnp.float32)).astype(jnp.bfloat16)

        dd_copy(n, k).wait()
        add(ochip)
        d2_copy(n, k).start()
        add(near)
        add(far)
        if k == 1:
            f_copy(n, 0).start()
            f_copy(n, 2).start()
        add(chip)

    def add_through(n):
        p = n % 2
        d2_copy(n, 0).wait_recv()
        pair[p, rchip, :, lo] = (pair[p, rchip, :, lo].astype(jnp.float32) + d2in[p, 0].astype(jnp.float32)).astype(jnp.bfloat16)
        f_copy(n, 1).start()
        d2_copy(n, 1).wait_recv()
        pair[p, lchip, :, hi] = (pair[p, lchip, :, hi].astype(jnp.float32) + d2in[p, 1].astype(jnp.float32)).astype(jnp.bfloat16)
        f_copy(n, 3).start()

    def finalize(n):
        for k in range(4):
            f_copy(n, k).wait_recv()
        p = n % 2
        f = n % 3
        b = n % n_seq
        o = pair[p, chip].astype(jnp.float32) + fin[f, 0].astype(jnp.float32) + fin[f, 1].astype(jnp.float32)
        o = o.astype(jnp.bfloat16).astype(jnp.float32)
        xo_ref[b] = (xo_ref[b].astype(jnp.float32) + o).astype(jnp.bfloat16)

    def forward_on(m):
        ag_wait_recv(m, (0,))
        ag_start(m, (5,))
        ag_wait_recv(m, (2,))
        ag_start(m, (6,))

    def forward_sib(m):
        ag_wait_recv(m, (1,))
        ag_start(m, (7,))
        ag_wait_recv(m, (3,))
        ag_start(m, (8,))

    def forward_far(m):
        ag_wait_recv(m, (5,))
        ag_start(m, (9,))
        ag_wait_recv(m, (6,))
        ag_start(m, (10,))

    def gathered(n):
        ag_wait_recv(n, (4, 7, 8, 9, 10))

    def event_add(n):
        @pl.when(n >= 1)
        def _():
            add_through(n - 1)

    def event_forward(n):
        @pl.when(n + 1 < steps)
        def _():
            forward_on(n + 1)

    def event_sib(n):
        @pl.when(n + 1 < steps)
        def _():
            forward_sib(n + 1)

    def event_far(n):
        @pl.when(n + 1 < steps)
        def _():
            forward_far(n + 1)

    def event_finalize(n):
        @pl.when(n >= 1)
        def _():
            finalize(n - 1)

            @pl.when(n + 2 < steps)
            def _():
                norm_into((n + 2) % n_seq, (n + 2) // n_seq, n + 2)
                ag_start(n + 2, range(5))

    def after_compute(n):
        pair_sum(n, 0)
        event_sib(n)
        pair_sum(n, 1)
        event_finalize(n)
        event_far(n)

    def rows_of(g):
        return gath[g].reshape(new_len, d_model)

    def put_part(cols, val):
        part[:, :, :, cols] = val.astype(jnp.bfloat16).reshape(CHIPS, CORES, tok, val.shape[-1])

    NT = (((1,), (1,)), ((), ()))
    tile = 256

    def product_into_part(n, c0, width, weights, between):
        quarter = half // 2
        for k in range(4):
            if k == 1:
                between(n)
            cols = pl.ds(k * quarter, quarter)
            put_part(cols, jnp.dot(abuf[:, pl.ds(c0, width)], weights[:, cols], preferred_element_type=jnp.float32))
            if k % 2:
                dd_copy(n, k // 2).start()

    def attn_step(l, b, n):
        a = l * n_seq + b
        p = a % 2
        wait(kv_loads(a))

        @pl.when(a + 1 < n_layers * n_seq)
        def _():
            start(kv_loads(a + 1))

        gathered(n)
        g = n % GSLOTS
        cos_t, sin_lo, sin_hi = cos_ref[b], slo_ref[b], shi_ref[b]
        quarter = head_dim // 4

        def rotate(val):
            return (val * cos_t + pltpu.roll(val, head_dim - quarter, 1) * sin_lo + pltpu.roll(val, quarter, 1) * sin_hi).astype(jnp.bfloat16)

        kv = jnp.dot(rows_of(g), wqkv[:, pl.ds(heads * head_dim, 2 * head_dim)], preferred_element_type=jnp.float32)
        kbuf[p, pl.ds(prefix, new_len)] = rotate(kv[:, :head_dim])
        vbuf[p, pl.ds(prefix, new_len)] = kv[:, head_dim:].astype(jnp.bfloat16)
        outs = [pltpu.make_async_copy(kbuf.at[p, pl.ds(prefix, new_len)], kn_ref.at[l, b], kn_sem.at[0]),
                pltpu.make_async_copy(vbuf.at[p, pl.ds(prefix, new_len)], vn_ref.at[l, b], kn_sem.at[1])]
        start(outs)

        @pl.loop(0, heads // 2)
        def _(j):
            q2 = jnp.dot(rows_of(g), wqkv[:, pl.ds(pl.multiple_of(j * tile, tile), tile)], preferred_element_type=jnp.float32)
            base = pl.multiple_of(j * tile, tile)
            abuf[:, pl.ds(base, head_dim)] = rotate(q2[:, :head_dim])
            abuf[:, pl.ds(base + head_dim, head_dim)] = rotate(q2[:, head_dim:])

        first_len = start_ref[b]
        chunk = prefix // 4
        chunks = [(c, chunk) for c in range(0, prefix, chunk)] + [(prefix, new_len)]
        c_exp = head_dim ** -0.5 * math.log2(math.e)
        neg = NEG_BIG * head_dim ** 0.5
        bufs = (sbuf_a, sbuf_b)

        def fold(old, val, op):
            for k in range(0, val.shape[-1], 128):
                piece = val[:, k:k + 128]
                old = piece if old is None else op(old, piece)
            return old

        def score_chunk(h, q, peak, c0, cl):
            s = lax.dot_general(q, kbuf[p, pl.ds(c0, cl)], NT, preferred_element_type=jnp.float32)
            if c0:
                col = lax.broadcasted_iota(jnp.int32, (new_len, cl), 1)
                last = lax.broadcasted_iota(jnp.int32, (new_len, cl), 0) if c0 >= prefix else first_len - c0 - 1
                s = jnp.where(col <= last, s, neg)
            bufs[h % 2][:, pl.ds(c0, cl)] = s
            return fold(peak, s, jnp.maximum)

        def weigh_chunk(h, peak, total, acc, c0, cl):
            e = jnp.exp2((bufs[h % 2][:, pl.ds(c0, cl)] - peak) * c_exp)
            part_ctx = jnp.dot(e.astype(jnp.bfloat16), vbuf[p, pl.ds(c0, cl)], preferred_element_type=jnp.float32)
            return fold(total, e, jnp.add), part_ctx if acc is None else acc + part_ctx

        peaks = None
        for h in range(heads + 1):
            if h == heads // 2:
                event_add(n)
            if h == heads:
                event_forward(n)
            q = abuf[:, pl.ds(h * head_dim, head_dim)] if h < heads else None
            next_peak = total = acc = None
            for c0, cl in chunks:
                if h < heads:
                    next_peak = score_chunk(h, q, next_peak, c0, cl)
                if h:
                    total, acc = weigh_chunk(h - 1, peaks, total, acc, c0, cl)
            if h:
                ctx = acc / jnp.sum(total, axis=-1, keepdims=True)
                abuf[:, pl.ds((heads + h - 1) * head_dim, head_dim)] = ctx.astype(jnp.bfloat16)
            if h < heads:
                peaks = jnp.max(next_peak, axis=-1, keepdims=True)

        product_into_part(n, heads * head_dim, heads * head_dim, wov, lambda n: None)
        wait(outs)
        after_compute(n)

    def mlp_step(n):
        gathered(n)
        g = n % GSLOTS

        def up(cols):
            val = jnp.dot(rows_of(g), wuv[:, cols], preferred_element_type=jnp.float32)
            val = jnp.maximum(val, 0.0)
            abuf[:, cols] = (val * val).astype(jnp.bfloat16)

        @pl.loop(0, ff // tile)
        def _(j):
            up(pl.ds(pl.multiple_of(j * tile, tile), tile))

        if ff % tile:
            up(pl.ds(ff - ff % tile, ff % tile))
        event_add(n)
        product_into_part(n, 0, ff, wdv, event_forward)
        after_compute(n)

    def affine(l, k):
        gain_ref[2 * l + k] = 1.0 + lng_ref[l, k:k + 1].astype(jnp.float32)
        bias_ref[2 * l + k] = lnb_ref[l, k:k + 1].astype(jnp.float32)

    barrier = pltpu.get_barrier_semaphore()
    for dev in (left, right, sibling):
        pl.semaphore_signal(barrier, inc=1, device_id=dev, device_id_type=pl.DeviceIdType.MESH)
    start(attn_weights(0))
    start(kv_loads(0))
    affine(0, 0)
    xo_ref[0] = x_ref[0]
    norm_into(0, 0, 0)
    pl.semaphore_wait(barrier, 3)
    ag_start(0, range(5))
    for b in range(1, n_seq):
        xo_ref[b] = x_ref[b]
        norm_into(b, 0, b)
    for i in range(1, 2 * n_layers):
        affine(i // 2, i % 2)

    lane = lax.broadcasted_iota(jnp.int32, (new_len, head_dim), 1)
    row = lax.broadcasted_iota(jnp.int32, (new_len, head_dim), 0)
    rot = head_dim // 2

    @pl.loop(0, n_seq)
    def _(b):
        angle = (start_ref[b] + row).astype(jnp.float32) * freq_ref[...]
        sin_a = jnp.sin(angle)
        cos_ref[b] = jnp.where(lane < rot, jnp.cos(angle), 1.0)
        slo_ref[b] = jnp.where(lane < rot // 2, -sin_a, 0.0)
        shi_ref[b] = jnp.where(jnp.logical_and(lane >= rot // 2, lane < rot), sin_a, 0.0)

    forward_on(0)
    ag_start(1, range(5))
    forward_sib(0)
    ag_start(2, range(5))
    forward_far(0)

    @pl.loop(0, n_layers)
    def _(l):
        wait(attn_weights(l))
        start(mlp_weights(l))

        @pl.loop(0, n_seq)
        def _(b):
            attn_step(l, b, l * 2 * n_seq + b)

        @pl.when(l + 1 < n_layers)
        def _():
            start(attn_weights(l + 1))

        wait(mlp_weights(l))

        @pl.loop(0, n_seq)
        def _(b):
            mlp_step(l * 2 * n_seq + n_seq + b)

    add_through(steps - 1)
    finalize(steps - 1)
    for n in (steps - 2, steps - 1):
        for k in range(2):
            d2_copy(n, k).wait_send()
        for k in range(4):
            f_copy(n, k).wait_send()


def run_layers(start_pos, x_loc, k_cache, v_cache, w_q, w_k, w_v, w_o, w_up, w_down, ln_gain, ln_bias, new_len):
    n_layers, n_seq, _, cache_len, head_dim = k_cache.shape
    tok, d_model = x_loc.shape[1:]
    heads = w_q.shape[2] // head_dim
    prefix = cache_len - new_len
    ff = w_up.shape[2]
    bf, f32 = jnp.bfloat16, jnp.float32
    vm = pl.BlockSpec(memory_space=pltpu.VMEM)
    hb = pl.BlockSpec(memory_space=pl.ANY)
    dims = (n_layers, n_seq, tok, d_model, heads, head_dim, prefix, ff)
    dma = pltpu.SemaphoreType.DMA
    return pl.pallas_call(
        functools.partial(layers_kernel, dims),
        out_shape=(jax.ShapeDtypeStruct(x_loc.shape, bf),
                   jax.ShapeDtypeStruct((n_layers, n_seq, new_len, head_dim), bf),
                   jax.ShapeDtypeStruct((n_layers, n_seq, new_len, head_dim), bf)),
        in_specs=[pl.BlockSpec(memory_space=pltpu.SMEM)] + [vm] * 4 + [hb] * 8,
        out_specs=(vm, hb, hb),
        scratch_shapes=[
            pltpu.VMEM((GSLOTS, CHIPS, CORES, tok, d_model), bf),
            pltpu.VMEM((CHIPS, CORES, tok, d_model), bf),
            pltpu.VMEM((2, CHIPS, tok, d_model), bf),
            pltpu.VMEM((2, CHIPS, tok, d_model), bf),
            pltpu.VMEM((2, 2, tok, d_model // 2), bf),
            pltpu.VMEM((3, 2, tok, d_model), bf),
            pltpu.VMEM((d_model, (heads + 2) * head_dim), bf),
            pltpu.VMEM((heads * head_dim, d_model), bf),
            pltpu.VMEM((d_model, ff), bf),
            pltpu.VMEM((ff, d_model), bf),
            pltpu.VMEM((2, cache_len, head_dim), bf),
            pltpu.VMEM((2, cache_len, head_dim), bf),
            pltpu.VMEM((new_len, max(ff, 2 * heads * head_dim)), bf),
            pltpu.VMEM((new_len, cache_len), f32),
            pltpu.VMEM((new_len, cache_len), f32),
            pltpu.VMEM((n_layers * 2, 1, d_model), f32),
            pltpu.VMEM((n_layers * 2, 1, d_model), f32),
            pltpu.VMEM((n_seq, new_len, head_dim), f32),
            pltpu.VMEM((n_seq, new_len, head_dim), f32),
            pltpu.VMEM((n_seq, new_len, head_dim), f32),
            dma((GSLOTS, 11)), dma((GSLOTS, 11)), dma((2, 2)), dma((2, 2)), dma((2, 2)), dma((2, 2)), dma((3, 4)), dma((3, 4)),
            dma((6,)), dma((2, 2)), dma((2,)),
        ],
        compiler_params=pltpu.CompilerParams(collective_id=0, has_side_effects=True, vmem_limit_bytes=67043328),
        name='layers',
    )(start_pos, x_loc, ln_gain, ln_bias, rope_freqs(head_dim), k_cache, v_cache, w_q, w_k, w_v, w_o, w_up, w_down)


def merge_kernel(dims, start_ref, x_ref, kc_ref, vc_ref, kn_ref, vn_ref, xo_ref, ko_ref, vo_ref,
                 xbuf, kbuf, vbuf, knew, vnew, x_sem, in_sem, new_sem, out_sem):
    blocks, n_seq, new_len, cache_len, head_dim = dims
    span = new_len + 16
    row = lax.broadcasted_iota(jnp.int32, (span, head_dim), 0)
    caches = ((kc_ref, kbuf, kn_ref, knew, ko_ref), (vc_ref, vbuf, vn_ref, vnew, vo_ref))

    def reads(i, c):
        old, buf, new, nbuf, _ = caches[c]
        return (pltpu.make_async_copy(old.at[i], buf.at[i], in_sem.at[i, c]),
                pltpu.make_async_copy(new.at[i], nbuf.at[i], new_sem.at[i, c]))

    def write(i, c):
        return pltpu.make_async_copy(caches[c][1].at[i], caches[c][4].at[i], out_sem.at[i, c])

    for i in range(blocks):
        for c in range(2):
            for copy in reads(i, c):
                copy.start()
    x_in = pltpu.make_async_copy(x_ref, xbuf, x_sem.at[0])
    x_out = pltpu.make_async_copy(xbuf, xo_ref, x_sem.at[1])
    x_in.start()

    @pl.loop(0, blocks)
    def _(i):
        first = start_ref[lax.rem(i, n_seq)]
        base = pl.multiple_of(jnp.minimum(first // 16 * 16, cache_len - span), 16)
        shift = first - base
        inside = jnp.logical_and(row >= shift, row < shift + new_len)
        for c in range(2):
            for copy in reads(i, c):
                copy.wait()
            _, buf, _, nbuf, _ = caches[c]
            fresh = jnp.concatenate([nbuf[i].astype(jnp.float32), jnp.zeros((16, head_dim), jnp.float32)], axis=0)
            fresh = pltpu.roll(fresh, shift, 0)
            kept = buf[i, pl.ds(base, span), :].astype(jnp.float32)
            buf[i, pl.ds(base, span), :] = jnp.where(inside, fresh, kept).astype(jnp.bfloat16)
            write(i, c).start()

    x_in.wait()
    x_out.start()

    @pl.loop(0, blocks)
    def _(i):
        for c in range(2):
            write(i, c).wait()

    x_out.wait()


def merge_caches(start_pos, hidden, k_cache, v_cache, k_new, v_new):
    n_layers, n_seq, kv, cache_len, head_dim = k_cache.shape
    new_len = k_new.shape[2]
    blocks = n_layers * n_seq
    bf = jnp.bfloat16
    flat = lambda c: c.reshape(blocks, cache_len, head_dim)
    flat_new = lambda c: c.reshape(blocks, new_len, head_dim)
    hb = pl.BlockSpec(memory_space=pl.ANY)
    shape = jax.ShapeDtypeStruct((blocks, cache_len, head_dim), bf)
    dma = pltpu.SemaphoreType.DMA
    x_out, k_out, v_out = pl.pallas_call(
        functools.partial(merge_kernel, (blocks, n_seq, new_len, cache_len, head_dim)),
        out_shape=(jax.ShapeDtypeStruct(hidden.shape, bf), shape, shape),
        in_specs=[pl.BlockSpec(memory_space=pltpu.SMEM)] + [hb] * 5,
        out_specs=(hb, hb, hb),
        scratch_shapes=[pltpu.VMEM(hidden.shape, bf), pltpu.VMEM((blocks, cache_len, head_dim), bf), pltpu.VMEM((blocks, cache_len, head_dim), bf),
                        pltpu.VMEM((blocks, new_len, head_dim), bf), pltpu.VMEM((blocks, new_len, head_dim), bf),
                        dma((2,)), dma((blocks, 2)), dma((blocks, 2)), dma((blocks, 2))],
        name='merge',
    )(start_pos, hidden, flat(k_cache), flat(v_cache), flat_new(k_new), flat_new(v_new))
    return x_out, k_out.reshape(k_cache.shape), v_out.reshape(v_cache.shape)


def solution(mesh):
    tp_size = mesh.shape['tp']
    assert tp_size == CORES * CHIPS
    tok_spec = P('dp', 'tp', None)
    cache_spec = P(None, 'dp', 'tp', None, None)
    col_spec = P(None, None, 'tp')
    row_spec = P(None, 'tp', None)

    def device_fn(x_loc, start_pos, k_cache, v_cache, w_q, w_k, w_v, w_o, w_up, w_down, ln_gain, ln_bias):
        hidden, k_new, v_new = run_layers(start_pos, x_loc, k_cache, v_cache, w_q, w_k, w_v, w_o, w_up, w_down, ln_gain, ln_bias, x_loc.shape[1] * tp_size)
        return merge_caches(start_pos, hidden, k_cache, v_cache, k_new, v_new)

    return jax.shard_map(device_fn, mesh=mesh, in_specs=(tok_spec, P('dp'), cache_spec, cache_spec, col_spec, col_spec, col_spec, row_spec, col_spec, row_spec, P(), P()), out_specs=(tok_spec, cache_spec, cache_spec), check_vma=False)
```

```python
import functools
import math

import jax
import jax.numpy as jnp
import numpy as np
from jax import lax
from jax.experimental import pallas as pl
from jax.experimental.pallas import tpu as pltpu
from jax.sharding import PartitionSpec as P

LN_EPS = 1e-5
ROPE_BASE = 10000.0
NEG_BIG = -1e30
CORES = 2
CHIPS = 4
GSLOTS = 3


def rope_freqs(head_dim):
    rot_dim = head_dim // 2
    half_rot = rot_dim // 2
    inv_freq = ROPE_BASE ** (-(np.arange(half_rot) * (2.0 / rot_dim)))
    return jnp.asarray(np.tile(inv_freq, head_dim // half_rot)[None].astype(np.float32))


def layers_kernel(dims, start_ref, x_ref, lng_ref, lnb_ref, freq_ref, kc_ref, vc_ref,
                  wq_ref, wk_ref, wv_ref, wo_ref, wu_ref, wd_ref,
                  xo_ref, kn_ref, vn_ref,
                  gath, part, pairin, pair, d2in, fin, wqkv, wov, wuv, wdv, kbuf, vbuf, abuf, sbuf_a, sbuf_b,
                  gain_ref, bias_ref, cos_ref, sin_ref,
                  ag_s, ag_r, dd_s, dd_r, d2_s, d2_r, f_s, f_r, w_sem, kv_sem, kn_sem):
    n_layers, n_seq, tok, d_model, heads, head_dim, prefix, ff = dims
    new_len = tok * CORES * CHIPS
    half = d_model // 2
    steps = n_layers * 2 * n_seq
    tp_idx = lax.axis_index('tp')
    chip = tp_idx // CORES
    core = tp_idx % CORES
    sib = 1 - core
    rchip = (chip + 1) % CHIPS
    lchip = (chip + CHIPS - 1) % CHIPS
    ochip = (chip + 2) % CHIPS
    right = {'tp': rchip * CORES + core}
    left = {'tp': lchip * CORES + core}
    sibling = {'tp': chip * CORES + sib}
    lo = pl.ds(0, half)
    hi = pl.ds(half, half)

    def remote(src, dst, s_sem, r_sem, dev):
        return pltpu.make_async_remote_copy(src_ref=src, dst_ref=dst, send_sem=s_sem, recv_sem=r_sem,
                                            device_id=dev, device_id_type=pl.DeviceIdType.MESH)

    def ag_copy(m, k):
        g = m % GSLOTS
        where_from = [(chip, core, lo, right), (chip, core, hi, right), (chip, core, hi, left), (chip, core, lo, left),
                      (chip, core, None, sibling), (lchip, core, lo, right), (rchip, core, hi, left),
                      (lchip, core, None, sibling), (rchip, core, None, sibling), (ochip, core, lo, sibling),
                      (ochip, core, hi, sibling)]
        c, r, cols, dev = where_from[k]
        ref = gath.at[g, c, r] if cols is None else gath.at[g, c, r, :, cols]
        return remote(ref, ref, ag_s.at[g, k], ag_r.at[g, k], dev)

    def ag_start(m, ks):
        for k in ks:
            ag_copy(m, k).start()

    def ag_wait_recv(m, ks):
        for k in ks:
            ag_copy(m, k).wait_recv()

    def dd_copy(n, k):
        p = n % 2
        cols = (lo, hi)[k]
        return remote(part.at[:, sib, :, cols], pairin.at[p, :, :, cols], dd_s.at[p, k], dd_r.at[p, k], sibling)

    def d2_copy(n, k):
        p = n % 2
        cols, dev = [(lo, right), (hi, left)][k]
        return remote(pair.at[p, ochip, :, cols], d2in.at[p, k], d2_s.at[p, k], d2_r.at[p, k], dev)

    def f_copy(n, k):
        p = n % 2
        f = n % 3
        c, cols, side, dev = [(rchip, hi, 0, right), (rchip, lo, 0, right), (lchip, lo, 1, left), (lchip, hi, 1, left)][k]
        return remote(pair.at[p, c, :, cols], fin.at[f, side, :, cols], f_s.at[f, k], f_r.at[f, k], dev)

    def attn_weights(l):
        qw = heads * head_dim
        return [pltpu.make_async_copy(wq_ref.at[l], wqkv.at[:, pl.ds(0, qw)], w_sem.at[0]),
                pltpu.make_async_copy(wk_ref.at[l], wqkv.at[:, pl.ds(qw, head_dim)], w_sem.at[1]),
                pltpu.make_async_copy(wv_ref.at[l], wqkv.at[:, pl.ds(qw + head_dim, head_dim)], w_sem.at[2]),
                pltpu.make_async_copy(wo_ref.at[l], wov, w_sem.at[3])]

    def mlp_weights(l):
        return [pltpu.make_async_copy(wu_ref.at[l], wuv, w_sem.at[4]),
                pltpu.make_async_copy(wd_ref.at[l], wdv, w_sem.at[5])]

    def kv_loads(a):
        l, b, p = a // n_seq, a % n_seq, a % 2
        rows = pl.ds(0, prefix)
        return [pltpu.make_async_copy(kc_ref.at[l, b, 0, rows], kbuf.at[p, rows], kv_sem.at[p, 0]),
                pltpu.make_async_copy(vc_ref.at[l, b, 0, rows], vbuf.at[p, rows], kv_sem.at[p, 1])]

    def start(copies):
        for c in copies:
            c.start()

    def wait(copies):
        for c in copies:
            c.wait()

    def norm_into(b, idx, m):
        xf = xo_ref[b].astype(jnp.float32)
        mean = jnp.sum(xf, axis=-1, keepdims=True) * (1.0 / d_model)
        cen = xf - mean
        var = jnp.sum(cen * cen, axis=-1, keepdims=True) * (1.0 / d_model)
        out = cen * lax.rsqrt(var + LN_EPS) * gain_ref[idx] + bias_ref[idx]
        gath[m % GSLOTS, chip, core] = out.astype(jnp.bfloat16)

    def ready_start(n):
        f_copy(n, 0).start()
        f_copy(n, 2).start()

    def pair_sum(n, k):
        if k == 0:
            for i in range(11):
                ag_copy(n, i).wait_send()

            @pl.when(n >= 2)
            def _():
                for i in range(2):
                    d2_copy(n - 2, i).wait_send()
                for i in range(4):
                    f_copy(n - 2, i).wait_send()

        p = n % 2
        cols, near, far = ((lo, lchip, rchip), (hi, rchip, lchip))[k]

        def add(c):
            pair[p, c, :, cols] = (part[c, core, :, cols].astype(jnp.float32) + pairin[p, c, :, cols].astype(jnp.float32)).astype(jnp.bfloat16)

        dd_copy(n, k).wait()
        add(ochip)
        d2_copy(n, k).start()
        add(near)
        add(far)
        if k == 1:
            @pl.when(jnp.logical_or(n < last_gather, n == steps - 1))
            def _():
                ready_start(n)

        add(chip)

    def add_through(n):
        p = n % 2
        for k, c, cols in ((0, rchip, lo), (1, lchip, hi)):
            d2_copy(n, k).wait_recv()
            pair[p, c, :, cols] = (pair[p, c, :, cols].astype(jnp.float32) + d2in[p, k].astype(jnp.float32)).astype(jnp.bfloat16)
        f_copy(n, 1).start()
        f_copy(n, 3).start()

    def finalize(n):
        for k in range(4):
            f_copy(n, k).wait_recv()
        p = n % 2
        f = n % 3
        b = n % n_seq
        o = pair[p, chip].astype(jnp.float32) + fin[f, 0].astype(jnp.float32) + fin[f, 1].astype(jnp.float32)
        o = o.astype(jnp.bfloat16).astype(jnp.float32)
        xo_ref[b] = (xo_ref[b].astype(jnp.float32) + o).astype(jnp.bfloat16)

    def forward_on(m):
        ag_wait_recv(m, (0,))
        ag_start(m, (5,))
        ag_wait_recv(m, (2,))
        ag_start(m, (6,))

    def forward_sib(m):
        ag_wait_recv(m, (1,))
        ag_start(m, (7,))
        ag_wait_recv(m, (3,))
        ag_start(m, (8,))

    def forward_far(m):
        ag_wait_recv(m, (5,))
        ag_start(m, (9,))
        ag_wait_recv(m, (6,))
        ag_start(m, (10,))

    def gathered(n):
        ag_wait_recv(n, (4, 7, 8, 9, 10))

    last_gather = steps - 3

    def event_add(n):
        @pl.when(jnp.logical_and(n >= 1, n <= last_gather))
        def _():
            add_through(n - 1)

    def event_forward(n):
        @pl.when(n + 1 < steps)
        def _():
            forward_on(n + 1)

    def event_sib(n):
        @pl.when(n + 1 < steps)
        def _():
            forward_sib(n + 1)

    def event_far(n):
        @pl.when(n + 1 < steps)
        def _():
            forward_far(n + 1)

    def event_finalize(n):
        @pl.when(n >= 1)
        def _():
            finalize(n - 1)

            @pl.when(n + 2 < steps)
            def _():
                norm_into((n + 2) % n_seq, (n + 2) // n_seq, n + 2)
                ag_start(n + 2, range(5))

    def after_compute(n):
        early = n <= n_seq - 2

        @pl.when(n == steps - 1)
        def _():
            add_through(n - 1)
            finalize(last_gather)

        pair_sum(n, 0)

        @pl.when(early)
        def _():
            event_far(n)

        @pl.when(jnp.logical_not(early))
        def _():
            event_sib(n)

        @pl.when(n == last_gather + 1)
        def _():
            ready_start(last_gather)
            add_through(last_gather)

        pair_sum(n, 1)

        @pl.when(n == last_gather + 1)
        def _():
            event_far(n)
            ready_start(n)

        @pl.when(n != last_gather + 1)
        def _():
            event_finalize(n)

            @pl.when(jnp.logical_not(early))
            def _():
                event_far(n)

    def rows_of(g):
        return gath[g].reshape(new_len, d_model)

    def put_part(cols, val):
        part[:, :, :, cols] = val.astype(jnp.bfloat16).reshape(CHIPS, CORES, tok, val.shape[-1])

    NT = (((1,), (1,)), ((), ()))
    tile = 256

    def product_into_part(n, c0, width, weights, between):
        quarter = half // 2
        for k in range(4):
            if k == 1:
                between(n)
            cols = pl.ds(k * quarter, quarter)
            put_part(cols, jnp.dot(abuf[:, pl.ds(c0, width)], weights[:, cols], preferred_element_type=jnp.float32))
            if k % 2:
                dd_copy(n, k // 2).start()

    def qkv(b, p, g):
        quarter = head_dim // 4
        lane = lax.broadcasted_iota(jnp.int32, (new_len, head_dim), 1)

        def rotate(val):
            other = jnp.where(lane < quarter, pltpu.roll(val, head_dim - quarter, 1), pltpu.roll(val, quarter, 1))
            return (val * cos_ref[b] + other * sin_ref[b]).astype(jnp.bfloat16)

        kv = jnp.dot(rows_of(g), wqkv[:, pl.ds(heads * head_dim, 2 * head_dim)], preferred_element_type=jnp.float32)
        kbuf[p, pl.ds(prefix, new_len)] = rotate(kv[:, :head_dim])
        vbuf[p, pl.ds(prefix, new_len)] = kv[:, head_dim:].astype(jnp.bfloat16)

        @pl.loop(0, heads // 2)
        def _(j):
            base = pl.multiple_of(j * tile, tile)
            q2 = jnp.dot(rows_of(g), wqkv[:, pl.ds(base, tile)], preferred_element_type=jnp.float32)
            abuf[:, pl.ds(base, head_dim)] = rotate(q2[:, :head_dim])
            abuf[:, pl.ds(base + head_dim, head_dim)] = rotate(q2[:, head_dim:])

    def attn_step(l, b, n):
        a = l * n_seq + b
        p = a % 2
        wait(kv_loads(a))

        @pl.when(a + 1 < n_layers * n_seq)
        def _():
            start(kv_loads(a + 1))

        gathered(n)
        qkv(b, p, n % GSLOTS)
        outs = [pltpu.make_async_copy(kbuf.at[p, pl.ds(prefix, new_len)], kn_ref.at[l, b], kn_sem.at[0]),
                pltpu.make_async_copy(vbuf.at[p, pl.ds(prefix, new_len)], vn_ref.at[l, b], kn_sem.at[1])]
        start(outs)

        early = n <= n_seq - 2
        first_len = start_ref[b]
        chunk = prefix // 4
        chunks = [(c, chunk) for c in range(0, prefix, chunk)] + [(prefix, new_len)]
        c_exp = head_dim ** -0.5 * math.log2(math.e)
        neg = NEG_BIG * head_dim ** 0.5
        bufs = (sbuf_a, sbuf_b)

        def fold(old, val, op):
            for k in range(0, val.shape[-1], 128):
                piece = val[:, k:k + 128]
                old = piece if old is None else op(old, piece)
            return old

        def score_chunk(h, q, peak, c0, cl):
            s = lax.dot_general(q, kbuf[p, pl.ds(c0, cl)], NT, preferred_element_type=jnp.float32)
            if c0:
                col = lax.broadcasted_iota(jnp.int32, (new_len, cl), 1)
                last = lax.broadcasted_iota(jnp.int32, (new_len, cl), 0) if c0 >= prefix else first_len - c0 - 1
                s = jnp.where(col <= last, s, neg)
            bufs[h % 2][:, pl.ds(c0, cl)] = s
            return fold(peak, s, jnp.maximum)

        def weigh_chunk(h, peak, total, acc, c0, cl):
            e = jnp.exp2((bufs[h % 2][:, pl.ds(c0, cl)] - peak) * c_exp)
            part_ctx = jnp.dot(e.astype(jnp.bfloat16), vbuf[p, pl.ds(c0, cl)], preferred_element_type=jnp.float32)
            return fold(total, e, jnp.add), part_ctx if acc is None else acc + part_ctx

        peaks = None
        for h in range(heads + 1):
            if h == 1:
                pl.when(early)(lambda: event_forward(n))
            if h == heads // 2:
                event_add(n)
                pl.when(early)(lambda: event_sib(n))
            if h == heads:
                pl.when(jnp.logical_not(early))(lambda: event_forward(n))
            q = abuf[:, pl.ds(h * head_dim, head_dim)] if h < heads else None
            next_peak = total = acc = None
            for c0, cl in chunks:
                if h < heads:
                    next_peak = score_chunk(h, q, next_peak, c0, cl)
                if h:
                    total, acc = weigh_chunk(h - 1, peaks, total, acc, c0, cl)
            if h:
                ctx = acc / jnp.sum(total, axis=-1, keepdims=True)
                abuf[:, pl.ds((heads + h - 1) * head_dim, head_dim)] = ctx.astype(jnp.bfloat16)
            if h < heads:
                peaks = jnp.max(next_peak, axis=-1, keepdims=True)

        product_into_part(n, heads * head_dim, heads * head_dim, wov, lambda n: None)
        wait(outs)
        after_compute(n)

    def mlp_step(n):
        gathered(n)
        g = n % GSLOTS

        def up(cols):
            val = jnp.dot(rows_of(g), wuv[:, cols], preferred_element_type=jnp.float32)
            val = jnp.maximum(val, 0.0)
            abuf[:, cols] = (val * val).astype(jnp.bfloat16)

        @pl.loop(0, ff // tile)
        def _(j):
            up(pl.ds(pl.multiple_of(j * tile, tile), tile))

        if ff % tile:
            up(pl.ds(ff - ff % tile, ff % tile))
        event_add(n)
        product_into_part(n, 0, ff, wdv, event_forward)
        after_compute(n)

    def affine(l, k):
        gain_ref[2 * l + k] = 1.0 + lng_ref[l, k:k + 1].astype(jnp.float32)
        bias_ref[2 * l + k] = lnb_ref[l, k:k + 1].astype(jnp.float32)

    barrier = pltpu.get_barrier_semaphore()
    for dev in (left, right, sibling):
        pl.semaphore_signal(barrier, inc=1, device_id=dev, device_id_type=pl.DeviceIdType.MESH)
    start(attn_weights(0))
    start(kv_loads(0))
    affine(0, 0)
    xo_ref[0] = x_ref[0]
    norm_into(0, 0, 0)
    pl.semaphore_wait(barrier, 3)
    ag_start(0, range(5))
    for b in range(1, n_seq):
        xo_ref[b] = x_ref[b]
        norm_into(b, 0, b)
    for i in range(1, 2 * n_layers):
        affine(i // 2, i % 2)

    lane = lax.broadcasted_iota(jnp.int32, (new_len, head_dim), 1)
    row = lax.broadcasted_iota(jnp.int32, (new_len, head_dim), 0)
    rot = head_dim // 2

    @pl.loop(0, n_seq)
    def _(b):
        angle = (start_ref[b] + row).astype(jnp.float32) * freq_ref[...]
        sin_a = jnp.sin(angle)
        cos_ref[b] = jnp.where(lane < rot, jnp.cos(angle), 1.0)
        sin_ref[b] = jnp.where(lane < rot // 2, -sin_a, jnp.where(lane < rot, sin_a, 0.0))

    forward_on(0)
    ag_start(1, range(5))
    forward_sib(0)
    ag_start(2, range(5))
    forward_far(0)

    @pl.loop(0, n_layers)
    def _(l):
        wait(attn_weights(l))
        start(mlp_weights(l))

        @pl.loop(0, n_seq)
        def _(b):
            attn_step(l, b, l * 2 * n_seq + b)

        @pl.when(l + 1 < n_layers)
        def _():
            start(attn_weights(l + 1))

        wait(mlp_weights(l))

        @pl.loop(0, n_seq)
        def _(b):
            mlp_step(l * 2 * n_seq + n_seq + b)

    add_through(steps - 1)
    finalize(steps - 1)
    for n in (steps - 2, steps - 1):
        for k in range(2):
            d2_copy(n, k).wait_send()
        for k in range(4):
            f_copy(n, k).wait_send()


def run_layers(start_pos, x_loc, k_cache, v_cache, w_q, w_k, w_v, w_o, w_up, w_down, ln_gain, ln_bias, new_len):
    n_layers, n_seq, _, cache_len, head_dim = k_cache.shape
    tok, d_model = x_loc.shape[1:]
    heads = w_q.shape[2] // head_dim
    prefix = cache_len - new_len
    ff = w_up.shape[2]
    bf, f32 = jnp.bfloat16, jnp.float32
    vm = pl.BlockSpec(memory_space=pltpu.VMEM)
    hb = pl.BlockSpec(memory_space=pl.ANY)
    dims = (n_layers, n_seq, tok, d_model, heads, head_dim, prefix, ff)
    dma = pltpu.SemaphoreType.DMA
    return pl.pallas_call(
        functools.partial(layers_kernel, dims),
        out_shape=(jax.ShapeDtypeStruct(x_loc.shape, bf),
                   jax.ShapeDtypeStruct((n_layers, n_seq, new_len, head_dim), bf),
                   jax.ShapeDtypeStruct((n_layers, n_seq, new_len, head_dim), bf)),
        in_specs=[pl.BlockSpec(memory_space=pltpu.SMEM)] + [vm] * 4 + [hb] * 8,
        out_specs=(vm, hb, hb),
        scratch_shapes=[
            pltpu.VMEM((GSLOTS, CHIPS, CORES, tok, d_model), bf),
            pltpu.VMEM((CHIPS, CORES, tok, d_model), bf),
            pltpu.VMEM((2, CHIPS, tok, d_model), bf),
            pltpu.VMEM((2, CHIPS, tok, d_model), bf),
            pltpu.VMEM((2, 2, tok, d_model // 2), bf),
            pltpu.VMEM((3, 2, tok, d_model), bf),
            pltpu.VMEM((d_model, (heads + 2) * head_dim), bf),
            pltpu.VMEM((heads * head_dim, d_model), bf),
            pltpu.VMEM((d_model, ff), bf),
            pltpu.VMEM((ff, d_model), bf),
            pltpu.VMEM((2, cache_len, head_dim), bf),
            pltpu.VMEM((2, cache_len, head_dim), bf),
            pltpu.VMEM((new_len, max(ff, 2 * heads * head_dim)), bf),
            pltpu.VMEM((new_len, cache_len), f32),
            pltpu.VMEM((new_len, cache_len), f32),
            pltpu.VMEM((n_layers * 2, 1, d_model), f32),
            pltpu.VMEM((n_layers * 2, 1, d_model), f32),
            pltpu.VMEM((n_seq, new_len, head_dim), f32),
            pltpu.VMEM((n_seq, new_len, head_dim), f32),
            dma((GSLOTS, 11)), dma((GSLOTS, 11)), dma((2, 2)), dma((2, 2)), dma((2, 2)), dma((2, 2)), dma((3, 4)), dma((3, 4)),
            dma((6,)), dma((2, 2)), dma((2,)),
        ],
        compiler_params=pltpu.CompilerParams(collective_id=0, has_side_effects=True, vmem_limit_bytes=67043328),
        name='layers',
    )(start_pos, x_loc, ln_gain, ln_bias, rope_freqs(head_dim), k_cache, v_cache, w_q, w_k, w_v, w_o, w_up, w_down)


def merge_kernel(dims, start_ref, x_ref, kc_ref, vc_ref, kn_ref, vn_ref, xo_ref, ko_ref, vo_ref,
                 xbuf, kbuf, vbuf, knew, vnew, x_sem, in_sem, new_sem, out_sem):
    blocks, n_seq, new_len, cache_len, head_dim = dims
    span = new_len + 16
    row = lax.broadcasted_iota(jnp.int32, (span, head_dim), 0)
    caches = ((kc_ref, kbuf, kn_ref, knew, ko_ref), (vc_ref, vbuf, vn_ref, vnew, vo_ref))

    def reads(i, c):
        old, buf, new, nbuf, _ = caches[c]
        return (pltpu.make_async_copy(old.at[i], buf.at[i], in_sem.at[i, c]),
                pltpu.make_async_copy(new.at[i], nbuf.at[i], new_sem.at[i, c]))

    def write(i, c):
        return pltpu.make_async_copy(caches[c][1].at[i], caches[c][4].at[i], out_sem.at[i, c])

    for i in range(blocks):
        for c in range(2):
            for copy in reads(i, c):
                copy.start()
    x_in = pltpu.make_async_copy(x_ref, xbuf, x_sem.at[0])
    x_out = pltpu.make_async_copy(xbuf, xo_ref, x_sem.at[1])
    x_in.start()

    @pl.loop(0, blocks)
    def _(i):
        first = start_ref[lax.rem(i, n_seq)]
        base = pl.multiple_of(jnp.minimum(first // 16 * 16, cache_len - span), 16)
        shift = first - base
        inside = jnp.logical_and(row >= shift, row < shift + new_len)
        for c in range(2):
            for copy in reads(i, c):
                copy.wait()
            _, buf, _, nbuf, _ = caches[c]
            fresh = jnp.concatenate([nbuf[i].astype(jnp.float32), jnp.zeros((16, head_dim), jnp.float32)], axis=0)
            fresh = pltpu.roll(fresh, shift, 0)
            kept = buf[i, pl.ds(base, span), :].astype(jnp.float32)
            buf[i, pl.ds(base, span), :] = jnp.where(inside, fresh, kept).astype(jnp.bfloat16)
            write(i, c).start()

    x_in.wait()
    x_out.start()

    @pl.loop(0, blocks)
    def _(i):
        for c in range(2):
            write(i, c).wait()

    x_out.wait()


def merge_caches(start_pos, hidden, k_cache, v_cache, k_new, v_new):
    n_layers, n_seq, kv, cache_len, head_dim = k_cache.shape
    new_len = k_new.shape[2]
    blocks = n_layers * n_seq
    bf = jnp.bfloat16
    flat = lambda c: c.reshape(blocks, cache_len, head_dim)
    flat_new = lambda c: c.reshape(blocks, new_len, head_dim)
    hb = pl.BlockSpec(memory_space=pl.ANY)
    shape = jax.ShapeDtypeStruct((blocks, cache_len, head_dim), bf)
    dma = pltpu.SemaphoreType.DMA
    x_out, k_out, v_out = pl.pallas_call(
        functools.partial(merge_kernel, (blocks, n_seq, new_len, cache_len, head_dim)),
        out_shape=(jax.ShapeDtypeStruct(hidden.shape, bf), shape, shape),
        in_specs=[pl.BlockSpec(memory_space=pltpu.SMEM)] + [hb] * 5,
        out_specs=(hb, hb, hb),
        scratch_shapes=[pltpu.VMEM(hidden.shape, bf), pltpu.VMEM((blocks, cache_len, head_dim), bf), pltpu.VMEM((blocks, cache_len, head_dim), bf),
                        pltpu.VMEM((blocks, new_len, head_dim), bf), pltpu.VMEM((blocks, new_len, head_dim), bf),
                        dma((2,)), dma((blocks, 2)), dma((blocks, 2)), dma((blocks, 2))],
        name='merge',
    )(start_pos, hidden, flat(k_cache), flat(v_cache), flat_new(k_new), flat_new(v_new))
    return x_out, k_out.reshape(k_cache.shape), v_out.reshape(v_cache.shape)


def solution(mesh):
    tp_size = mesh.shape['tp']
    assert tp_size == CORES * CHIPS
    tok_spec = P('dp', 'tp', None)
    cache_spec = P(None, 'dp', 'tp', None, None)
    col_spec = P(None, None, 'tp')
    row_spec = P(None, 'tp', None)

    def device_fn(x_loc, start_pos, k_cache, v_cache, w_q, w_k, w_v, w_o, w_up, w_down, ln_gain, ln_bias):
        hidden, k_new, v_new = run_layers(start_pos, x_loc, k_cache, v_cache, w_q, w_k, w_v, w_o, w_up, w_down, ln_gain, ln_bias, x_loc.shape[1] * tp_size)
        return merge_caches(start_pos, hidden, k_cache, v_cache, k_new, v_new)

    return jax.shard_map(device_fn, mesh=mesh, in_specs=(tok_spec, P('dp'), cache_spec, cache_spec, col_spec, col_spec, col_spec, row_spec, col_spec, row_spec, P(), P()), out_specs=(tok_spec, cache_spec, cache_spec), check_vma=False)
```

```python
import functools
import math

import jax
import jax.numpy as jnp
import numpy as np
from jax import lax
from jax.experimental import pallas as pl
from jax.experimental.pallas import tpu as pltpu
from jax.sharding import PartitionSpec as P

LN_EPS = 1e-5
ROPE_BASE = 10000.0
NEG_BIG = -1e30
CORES = 2
CHIPS = 4
GSLOTS = 3


def rope_freqs(head_dim):
    rot_dim = head_dim // 2
    half_rot = rot_dim // 2
    inv_freq = ROPE_BASE ** (-(np.arange(half_rot) * (2.0 / rot_dim)))
    return jnp.asarray(np.tile(inv_freq, head_dim // half_rot)[None].astype(np.float32))


def layers_kernel(dims, start_ref, x_ref, lng_ref, lnb_ref, freq_ref, kc_ref, vc_ref,
                  wq_ref, wk_ref, wv_ref, wo_ref, wu_ref, wd_ref,
                  xo_ref, kn_ref, vn_ref,
                  gath, part, pairin, pair, d2in, fin, wqkv, wov, wuv, wdv, kbuf, vbuf, abuf, sbuf_a, sbuf_b,
                  gain_ref, bias_ref, cos_ref, sin_ref,
                  ag_s, ag_r, dd_s, dd_r, d2_s, d2_r, f_s, f_r, w_sem, kv_sem, kn_sem):
    n_layers, n_seq, tok, d_model, heads, head_dim, prefix, ff = dims
    new_len = tok * CORES * CHIPS
    half = d_model // 2
    steps = n_layers * 2 * n_seq
    tp_idx = lax.axis_index('tp')
    chip = tp_idx // CORES
    core = tp_idx % CORES
    sib = 1 - core
    rchip = (chip + 1) % CHIPS
    lchip = (chip + CHIPS - 1) % CHIPS
    ochip = (chip + 2) % CHIPS
    right = {'tp': rchip * CORES + core}
    left = {'tp': lchip * CORES + core}
    sibling = {'tp': chip * CORES + sib}
    lo = pl.ds(0, half)
    hi = pl.ds(half, half)

    def remote(src, dst, s_sem, r_sem, dev):
        return pltpu.make_async_remote_copy(src_ref=src, dst_ref=dst, send_sem=s_sem, recv_sem=r_sem,
                                            device_id=dev, device_id_type=pl.DeviceIdType.MESH)

    def ag_copy(m, k):
        g = m % GSLOTS
        where_from = [(chip, core, lo, right), (chip, core, hi, right), (chip, core, hi, left), (chip, core, lo, left),
                      (chip, core, None, sibling), (lchip, core, lo, right), (rchip, core, hi, left),
                      (lchip, core, None, sibling), (rchip, core, None, sibling), (ochip, core, lo, sibling),
                      (ochip, core, hi, sibling)]
        c, r, cols, dev = where_from[k]
        ref = gath.at[g, c, r] if cols is None else gath.at[g, c, r, :, cols]
        return remote(ref, ref, ag_s.at[g, k], ag_r.at[g, k], dev)

    def ag_start(m, ks):
        for k in ks:
            ag_copy(m, k).start()

    def ag_wait_recv(m, ks):
        for k in ks:
            ag_copy(m, k).wait_recv()

    def dd_copy(n, k):
        p = n % 2
        cols = (lo, hi)[k]
        return remote(part.at[:, sib, :, cols], pairin.at[p, :, :, cols], dd_s.at[p, k], dd_r.at[p, k], sibling)

    def d2_copy(n, k):
        p = n % 2
        cols, dev = [(lo, right), (hi, left)][k]
        return remote(pair.at[p, ochip, :, cols], d2in.at[p, k], d2_s.at[p, k], d2_r.at[p, k], dev)

    def f_copy(n, k):
        p = n % 2
        f = n % 3
        c, cols, side, dev = [(rchip, hi, 0, right), (rchip, lo, 0, right), (lchip, lo, 1, left), (lchip, hi, 1, left)][k]
        return remote(pair.at[p, c, :, cols], fin.at[f, side, :, cols], f_s.at[f, k], f_r.at[f, k], dev)

    def attn_weights(l):
        qw = heads * head_dim
        return [pltpu.make_async_copy(wq_ref.at[l], wqkv.at[:, pl.ds(0, qw)], w_sem.at[0]),
                pltpu.make_async_copy(wk_ref.at[l], wqkv.at[:, pl.ds(qw, head_dim)], w_sem.at[1]),
                pltpu.make_async_copy(wv_ref.at[l], wqkv.at[:, pl.ds(qw + head_dim, head_dim)], w_sem.at[2]),
                pltpu.make_async_copy(wo_ref.at[l], wov, w_sem.at[3])]

    def mlp_weights(l):
        return [pltpu.make_async_copy(wu_ref.at[l], wuv, w_sem.at[4]),
                pltpu.make_async_copy(wd_ref.at[l], wdv, w_sem.at[5])]

    def kv_loads(a):
        l, b, p = a // n_seq, a % n_seq, a % 2
        rows = pl.ds(0, prefix)
        return [pltpu.make_async_copy(kc_ref.at[l, b, 0, rows], kbuf.at[p, rows], kv_sem.at[p, 0]),
                pltpu.make_async_copy(vc_ref.at[l, b, 0, rows], vbuf.at[p, rows], kv_sem.at[p, 1])]

    def start(copies):
        for c in copies:
            c.start()

    def wait(copies):
        for c in copies:
            c.wait()

    def norm_into(b, idx, m):
        xf = xo_ref[b].astype(jnp.float32)
        mean = jnp.sum(xf, axis=-1, keepdims=True) * (1.0 / d_model)
        cen = xf - mean
        var = jnp.sum(cen * cen, axis=-1, keepdims=True) * (1.0 / d_model)
        out = cen * lax.rsqrt(var + LN_EPS) * gain_ref[idx] + bias_ref[idx]
        gath[m % GSLOTS, chip, core] = out.astype(jnp.bfloat16)

    def ready_start(n):
        f_copy(n, 0).start()
        f_copy(n, 2).start()

    def pair_sum(n, k):
        if k == 0:
            for i in range(11):
                ag_copy(n, i).wait_send()

            @pl.when(n >= 2)
            def _():
                for i in range(2):
                    d2_copy(n - 2, i).wait_send()
                for i in range(4):
                    f_copy(n - 2, i).wait_send()

        p = n % 2
        cols, near, far = ((lo, lchip, rchip), (hi, rchip, lchip))[k]

        def add(c):
            pair[p, c, :, cols] = (part[c, core, :, cols].astype(jnp.float32) + pairin[p, c, :, cols].astype(jnp.float32)).astype(jnp.bfloat16)

        dd_copy(n, k).wait()
        add(ochip)
        d2_copy(n, k).start()
        add(near)
        add(far)
        if k == 1:
            @pl.when(jnp.logical_or(n < last_gather, n == steps - 1))
            def _():
                ready_start(n)

        add(chip)

    def add_through(n):
        p = n % 2
        for k, c, cols in ((0, rchip, lo), (1, lchip, hi)):
            d2_copy(n, k).wait_recv()
            pair[p, c, :, cols] = (pair[p, c, :, cols].astype(jnp.float32) + d2in[p, k].astype(jnp.float32)).astype(jnp.bfloat16)
        f_copy(n, 1).start()
        f_copy(n, 3).start()

    def finalize(n):
        for k in range(4):
            f_copy(n, k).wait_recv()
        p = n % 2
        f = n % 3
        b = n % n_seq
        o = pair[p, chip].astype(jnp.float32) + fin[f, 0].astype(jnp.float32) + fin[f, 1].astype(jnp.float32)
        o = o.astype(jnp.bfloat16).astype(jnp.float32)
        xo_ref[b] = (xo_ref[b].astype(jnp.float32) + o).astype(jnp.bfloat16)

    def forward_on(m):
        ag_wait_recv(m, (0,))
        ag_start(m, (5,))
        ag_wait_recv(m, (2,))
        ag_start(m, (6,))

    def forward_sib(m):
        ag_wait_recv(m, (1,))
        ag_start(m, (7,))
        ag_wait_recv(m, (3,))
        ag_start(m, (8,))

    def forward_far(m):
        ag_wait_recv(m, (5,))
        ag_start(m, (9,))
        ag_wait_recv(m, (6,))
        ag_start(m, (10,))

    def gathered(n):
        ag_wait_recv(n, (4, 7, 8, 9, 10))

    last_gather = steps - 3

    def event_add(n):
        @pl.when(jnp.logical_and(n >= 1, n <= last_gather))
        def _():
            add_through(n - 1)

    def event_forward(n):
        @pl.when(n + 1 < steps)
        def _():
            forward_on(n + 1)

    def event_sib(n):
        @pl.when(n + 1 < steps)
        def _():
            forward_sib(n + 1)

    def event_far(n):
        @pl.when(n + 1 < steps)
        def _():
            forward_far(n + 1)

    def event_finalize(n):
        @pl.when(n >= 1)
        def _():
            finalize(n - 1)

            @pl.when(n + 2 < steps)
            def _():
                norm_into((n + 2) % n_seq, (n + 2) // n_seq, n + 2)
                ag_start(n + 2, range(5))

    def after_compute(n):
        early = n <= n_seq - 2

        @pl.when(n == steps - 1)
        def _():
            add_through(n - 1)
            finalize(last_gather)

        pair_sum(n, 0)

        @pl.when(early)
        def _():
            event_far(n)

        @pl.when(jnp.logical_not(early))
        def _():
            event_sib(n)

        @pl.when(n == last_gather + 1)
        def _():
            ready_start(last_gather)
            add_through(last_gather)

        pair_sum(n, 1)

        @pl.when(n == last_gather + 1)
        def _():
            event_far(n)
            ready_start(n)

        @pl.when(n != last_gather + 1)
        def _():
            event_finalize(n)

            @pl.when(jnp.logical_not(early))
            def _():
                event_far(n)

    def rows_of(g):
        return gath[g].reshape(new_len, d_model)

    def put_part(cols, val):
        part[:, :, :, cols] = val.astype(jnp.bfloat16).reshape(CHIPS, CORES, tok, val.shape[-1])

    NT = (((1,), (1,)), ((), ()))
    tile = 256

    def product_into_part(n, c0, width, weights, between):
        quarter = half // 2
        for k in range(4):
            if k == 1:
                between(n)
            cols = pl.ds(k * quarter, quarter)
            put_part(cols, jnp.dot(abuf[:, pl.ds(c0, width)], weights[:, cols], preferred_element_type=jnp.float32))
            if k % 2:
                dd_copy(n, k // 2).start()

    def qkv(b, p, g):
        quarter = head_dim // 4
        lane = lax.broadcasted_iota(jnp.int32, (new_len, head_dim), 1)

        def rotate(val):
            other = jnp.where(lane < quarter, pltpu.roll(val, head_dim - quarter, 1), pltpu.roll(val, quarter, 1))
            return (val * cos_ref[b] + other * sin_ref[b]).astype(jnp.bfloat16)

        kv = jnp.dot(rows_of(g), wqkv[:, pl.ds(heads * head_dim, 2 * head_dim)], preferred_element_type=jnp.float32)
        kbuf[p, pl.ds(prefix, new_len)] = rotate(kv[:, :head_dim])
        vbuf[p, pl.ds(prefix, new_len)] = kv[:, head_dim:].astype(jnp.bfloat16)

        for base in range(0, heads * head_dim, tile):
            q2 = jnp.dot(rows_of(g), wqkv[:, pl.ds(base, tile)], preferred_element_type=jnp.float32)
            abuf[:, pl.ds(base, head_dim)] = rotate(q2[:, :head_dim])
            abuf[:, pl.ds(base + head_dim, head_dim)] = rotate(q2[:, head_dim:])

    def attn_step(l, b, n):
        a = l * n_seq + b
        p = a % 2
        wait(kv_loads(a))

        @pl.when(a + 1 < n_layers * n_seq)
        def _():
            start(kv_loads(a + 1))

        gathered(n)
        qkv(b, p, n % GSLOTS)
        outs = [pltpu.make_async_copy(kbuf.at[p, pl.ds(prefix, new_len)], kn_ref.at[l, b], kn_sem.at[0]),
                pltpu.make_async_copy(vbuf.at[p, pl.ds(prefix, new_len)], vn_ref.at[l, b], kn_sem.at[1])]
        start(outs)

        early = n <= n_seq - 2
        first_len = start_ref[b]
        chunk = prefix // 4
        chunks = [(c, chunk) for c in range(0, prefix, chunk)] + [(prefix, new_len)]
        c_exp = head_dim ** -0.5 * math.log2(math.e)
        neg = NEG_BIG * head_dim ** 0.5
        bufs = (sbuf_a, sbuf_b)

        def fold(old, val, op):
            for k in range(0, val.shape[-1], 128):
                piece = val[:, k:k + 128]
                old = piece if old is None else op(old, piece)
            return old

        def score_chunk(h, q, peak, c0, cl):
            s = lax.dot_general(q, kbuf[p, pl.ds(c0, cl)], NT, preferred_element_type=jnp.float32)
            if c0:
                col = lax.broadcasted_iota(jnp.int32, (new_len, cl), 1)
                last = lax.broadcasted_iota(jnp.int32, (new_len, cl), 0) if c0 >= prefix else first_len - c0 - 1
                s = jnp.where(col <= last, s, neg)
            bufs[h % 2][:, pl.ds(c0, cl)] = s
            return fold(peak, s, jnp.maximum)

        def weigh_chunk(h, peak, total, acc, c0, cl):
            e = jnp.exp2((bufs[h % 2][:, pl.ds(c0, cl)] - peak) * c_exp)
            part_ctx = jnp.dot(e.astype(jnp.bfloat16), vbuf[p, pl.ds(c0, cl)], preferred_element_type=jnp.float32)
            return fold(total, e, jnp.add), part_ctx if acc is None else acc + part_ctx

        peaks = None
        for h in range(heads + 1):
            if h == 1:
                pl.when(early)(lambda: event_forward(n))
            if h == heads // 2:
                event_add(n)
                pl.when(early)(lambda: event_sib(n))
            if h == heads:
                pl.when(jnp.logical_not(early))(lambda: event_forward(n))
            q = abuf[:, pl.ds(h * head_dim, head_dim)] if h < heads else None
            next_peak = total = acc = None
            for c0, cl in chunks:
                if h < heads:
                    next_peak = score_chunk(h, q, next_peak, c0, cl)
                if h:
                    total, acc = weigh_chunk(h - 1, peaks, total, acc, c0, cl)
            if h:
                ctx = acc / jnp.sum(total, axis=-1, keepdims=True)
                abuf[:, pl.ds((heads + h - 1) * head_dim, head_dim)] = ctx.astype(jnp.bfloat16)
            if h < heads:
                peaks = jnp.max(next_peak, axis=-1, keepdims=True)

        product_into_part(n, heads * head_dim, heads * head_dim, wov, lambda n: None)
        wait(outs)
        after_compute(n)

    def mlp_step(n):
        gathered(n)
        g = n % GSLOTS

        def up(cols):
            val = jnp.dot(rows_of(g), wuv[:, cols], preferred_element_type=jnp.float32)
            val = jnp.maximum(val, 0.0)
            abuf[:, cols] = (val * val).astype(jnp.bfloat16)

        for c0 in range(0, ff, 2 * tile):
            up(pl.ds(c0, min(2 * tile, ff - c0)))

        event_add(n)
        product_into_part(n, 0, ff, wdv, event_forward)
        after_compute(n)

    def affine(l, k):
        gain_ref[2 * l + k] = 1.0 + lng_ref[l, k:k + 1].astype(jnp.float32)
        bias_ref[2 * l + k] = lnb_ref[l, k:k + 1].astype(jnp.float32)

    barrier = pltpu.get_barrier_semaphore()
    for dev in (left, right, sibling):
        pl.semaphore_signal(barrier, inc=1, device_id=dev, device_id_type=pl.DeviceIdType.MESH)
    start(attn_weights(0))
    start(kv_loads(0))
    affine(0, 0)
    xo_ref[0] = x_ref[0]
    norm_into(0, 0, 0)
    pl.semaphore_wait(barrier, 3)
    ag_start(0, range(5))
    for b in range(1, n_seq):
        xo_ref[b] = x_ref[b]
        norm_into(b, 0, b)
    for i in range(1, 2 * n_layers):
        affine(i // 2, i % 2)

    lane = lax.broadcasted_iota(jnp.int32, (new_len, head_dim), 1)
    row = lax.broadcasted_iota(jnp.int32, (new_len, head_dim), 0)
    rot = head_dim // 2

    @pl.loop(0, n_seq)
    def _(b):
        angle = (start_ref[b] + row).astype(jnp.float32) * freq_ref[...]
        sin_a = jnp.sin(angle)
        cos_ref[b] = jnp.where(lane < rot, jnp.cos(angle), 1.0)
        sin_ref[b] = jnp.where(lane < rot // 2, -sin_a, jnp.where(lane < rot, sin_a, 0.0))

    forward_on(0)
    ag_start(1, range(5))
    forward_sib(0)
    ag_start(2, range(5))
    forward_far(0)

    @pl.loop(0, n_layers)
    def _(l):
        wait(attn_weights(l))
        start(mlp_weights(l))

        @pl.loop(0, n_seq)
        def _(b):
            attn_step(l, b, l * 2 * n_seq + b)

        @pl.when(l + 1 < n_layers)
        def _():
            start(attn_weights(l + 1))

        wait(mlp_weights(l))

        @pl.loop(0, n_seq)
        def _(b):
            mlp_step(l * 2 * n_seq + n_seq + b)

    add_through(steps - 1)
    finalize(steps - 1)
    for n in (steps - 2, steps - 1):
        for k in range(2):
            d2_copy(n, k).wait_send()
        for k in range(4):
            f_copy(n, k).wait_send()


def run_layers(start_pos, x_loc, k_cache, v_cache, w_q, w_k, w_v, w_o, w_up, w_down, ln_gain, ln_bias, new_len):
    n_layers, n_seq, _, cache_len, head_dim = k_cache.shape
    tok, d_model = x_loc.shape[1:]
    heads = w_q.shape[2] // head_dim
    prefix = cache_len - new_len
    ff = w_up.shape[2]
    bf, f32 = jnp.bfloat16, jnp.float32
    vm = pl.BlockSpec(memory_space=pltpu.VMEM)
    hb = pl.BlockSpec(memory_space=pl.ANY)
    dims = (n_layers, n_seq, tok, d_model, heads, head_dim, prefix, ff)
    dma = pltpu.SemaphoreType.DMA
    return pl.pallas_call(
        functools.partial(layers_kernel, dims),
        out_shape=(jax.ShapeDtypeStruct(x_loc.shape, bf),
                   jax.ShapeDtypeStruct((n_layers, n_seq, new_len, head_dim), bf),
                   jax.ShapeDtypeStruct((n_layers, n_seq, new_len, head_dim), bf)),
        in_specs=[pl.BlockSpec(memory_space=pltpu.SMEM)] + [vm] * 4 + [hb] * 8,
        out_specs=(vm, hb, hb),
        scratch_shapes=[
            pltpu.VMEM((GSLOTS, CHIPS, CORES, tok, d_model), bf),
            pltpu.VMEM((CHIPS, CORES, tok, d_model), bf),
            pltpu.VMEM((2, CHIPS, tok, d_model), bf),
            pltpu.VMEM((2, CHIPS, tok, d_model), bf),
            pltpu.VMEM((2, 2, tok, d_model // 2), bf),
            pltpu.VMEM((3, 2, tok, d_model), bf),
            pltpu.VMEM((d_model, (heads + 2) * head_dim), bf),
            pltpu.VMEM((heads * head_dim, d_model), bf),
            pltpu.VMEM((d_model, ff), bf),
            pltpu.VMEM((ff, d_model), bf),
            pltpu.VMEM((2, cache_len, head_dim), bf),
            pltpu.VMEM((2, cache_len, head_dim), bf),
            pltpu.VMEM((new_len, max(ff, 2 * heads * head_dim)), bf),
            pltpu.VMEM((new_len, cache_len), f32),
            pltpu.VMEM((new_len, cache_len), f32),
            pltpu.VMEM((n_layers * 2, 1, d_model), f32),
            pltpu.VMEM((n_layers * 2, 1, d_model), f32),
            pltpu.VMEM((n_seq, new_len, head_dim), f32),
            pltpu.VMEM((n_seq, new_len, head_dim), f32),
            dma((GSLOTS, 11)), dma((GSLOTS, 11)), dma((2, 2)), dma((2, 2)), dma((2, 2)), dma((2, 2)), dma((3, 4)), dma((3, 4)),
            dma((6,)), dma((2, 2)), dma((2,)),
        ],
        compiler_params=pltpu.CompilerParams(collective_id=0, has_side_effects=True, vmem_limit_bytes=67043328),
        name='layers',
    )(start_pos, x_loc, ln_gain, ln_bias, rope_freqs(head_dim), k_cache, v_cache, w_q, w_k, w_v, w_o, w_up, w_down)


def merge_kernel(dims, start_ref, x_ref, kc_ref, vc_ref, kn_ref, vn_ref, xo_ref, ko_ref, vo_ref,
                 xbuf, kbuf, vbuf, knew, vnew, x_sem, in_sem, new_sem, out_sem):
    blocks, n_seq, new_len, cache_len, head_dim = dims
    span = new_len + 16
    row = lax.broadcasted_iota(jnp.int32, (span, head_dim), 0)
    caches = ((kc_ref, kbuf, kn_ref, knew, ko_ref), (vc_ref, vbuf, vn_ref, vnew, vo_ref))

    def reads(i, c):
        old, buf, new, nbuf, _ = caches[c]
        return (pltpu.make_async_copy(old.at[i], buf.at[i], in_sem.at[i, c]),
                pltpu.make_async_copy(new.at[i], nbuf.at[i], new_sem.at[i, c]))

    def write(i, c):
        return pltpu.make_async_copy(caches[c][1].at[i], caches[c][4].at[i], out_sem.at[i, c])

    for i in range(blocks):
        for c in range(2):
            for copy in reads(i, c):
                copy.start()
    x_in = pltpu.make_async_copy(x_ref, xbuf, x_sem.at[0])
    x_out = pltpu.make_async_copy(xbuf, xo_ref, x_sem.at[1])
    x_in.start()

    @pl.loop(0, blocks)
    def _(i):
        first = start_ref[lax.rem(i, n_seq)]
        base = pl.multiple_of(jnp.minimum(first // 16 * 16, cache_len - span), 16)
        shift = first - base
        inside = jnp.logical_and(row >= shift, row < shift + new_len)
        for c in range(2):
            for copy in reads(i, c):
                copy.wait()
            _, buf, _, nbuf, _ = caches[c]
            fresh = jnp.concatenate([nbuf[i].astype(jnp.float32), jnp.zeros((16, head_dim), jnp.float32)], axis=0)
            fresh = pltpu.roll(fresh, shift, 0)
            kept = buf[i, pl.ds(base, span), :].astype(jnp.float32)
            buf[i, pl.ds(base, span), :] = jnp.where(inside, fresh, kept).astype(jnp.bfloat16)
            write(i, c).start()

    x_in.wait()
    x_out.start()

    @pl.loop(0, blocks)
    def _(i):
        for c in range(2):
            write(i, c).wait()

    x_out.wait()


def merge_caches(start_pos, hidden, k_cache, v_cache, k_new, v_new):
    n_layers, n_seq, kv, cache_len, head_dim = k_cache.shape
    new_len = k_new.shape[2]
    blocks = n_layers * n_seq
    bf = jnp.bfloat16
    flat = lambda c: c.reshape(blocks, cache_len, head_dim)
    flat_new = lambda c: c.reshape(blocks, new_len, head_dim)
    hb = pl.BlockSpec(memory_space=pl.ANY)
    shape = jax.ShapeDtypeStruct((blocks, cache_len, head_dim), bf)
    dma = pltpu.SemaphoreType.DMA
    x_out, k_out, v_out = pl.pallas_call(
        functools.partial(merge_kernel, (blocks, n_seq, new_len, cache_len, head_dim)),
        out_shape=(jax.ShapeDtypeStruct(hidden.shape, bf), shape, shape),
        in_specs=[pl.BlockSpec(memory_space=pltpu.SMEM)] + [hb] * 5,
        out_specs=(hb, hb, hb),
        scratch_shapes=[pltpu.VMEM(hidden.shape, bf), pltpu.VMEM((blocks, cache_len, head_dim), bf), pltpu.VMEM((blocks, cache_len, head_dim), bf),
                        pltpu.VMEM((blocks, new_len, head_dim), bf), pltpu.VMEM((blocks, new_len, head_dim), bf),
                        dma((2,)), dma((blocks, 2)), dma((blocks, 2)), dma((blocks, 2))],
        name='merge',
    )(start_pos, hidden, flat(k_cache), flat(v_cache), flat_new(k_new), flat_new(v_new))
    return x_out, k_out.reshape(k_cache.shape), v_out.reshape(v_cache.shape)


def solution(mesh):
    tp_size = mesh.shape['tp']
    assert tp_size == CORES * CHIPS
    tok_spec = P('dp', 'tp', None)
    cache_spec = P(None, 'dp', 'tp', None, None)
    col_spec = P(None, None, 'tp')
    row_spec = P(None, 'tp', None)

    def device_fn(x_loc, start_pos, k_cache, v_cache, w_q, w_k, w_v, w_o, w_up, w_down, ln_gain, ln_bias):
        hidden, k_new, v_new = run_layers(start_pos, x_loc, k_cache, v_cache, w_q, w_k, w_v, w_o, w_up, w_down, ln_gain, ln_bias, x_loc.shape[1] * tp_size)
        return merge_caches(start_pos, hidden, k_cache, v_cache, k_new, v_new)

    return jax.shard_map(device_fn, mesh=mesh, in_specs=(tok_spec, P('dp'), cache_spec, cache_spec, col_spec, col_spec, col_spec, row_spec, col_spec, row_spec, P(), P()), out_specs=(tok_spec, cache_spec, cache_spec), check_vma=False)
```
